32 devices in a mesh: shard: 16 (over z, y, x), replica: 2 (over core).
Axes of the slice: x: 2, y: 2, z: 4, core: 2. Of those that a mesh axis runs over, the one named last changes fastest.
Arguments:
- request_rows: int32 [2, 16, 128], P('replica', 'shard'), may hold values from 0 to 1023, as said below
- token_slot: int32 [2, 2048], P('replica', 'shard'), may hold values from 0 to 127, as said below
- seq_lengths: int32 [2, 16, 8], P('replica', 'shard'), may hold values from 1 to 48, 128 in all within a row
- cotangent: bfloat16 [2, 2048, 256], P('replica', 'shard'), may hold values from -6 to 6
- table_slab: float32 [16384, 256], P('shard'), may hold values from -6 to 6
- adagrad_state: float32 [16384], P('shard'), may hold values from 0.1 to 1
- w_uvqk: bfloat16 [256, 1024], replicated, may hold values from -0.375 to 0.375
- w_out: bfloat16 [256, 256], replicated, may hold values from -0.375 to 0.375
- norm_gain: float32 [256], replicated, may hold values from 0.1 to 1.9
- out_gain: float32 [256], replicated, may hold values from 0.1 to 1.9
Outputs:
- row_update: float32 [16384, 256], P('shard')
- state_new: float32 [16384], P('shard')
- grad_uvqk: float32 [256, 1024], replicated
- grad_out: float32 [256, 256], replicated
- grad_gains: float32 [2, 256], replicated
The draws below stay inside these ranges and needn't reach their ends.
Inputs may be any that keep to these rules, and one draw needn't show every extreme that they name: `request_rows`: on each device the rows asked of one owner (slots j with one value of j // 8) are distinct. `token_slot`: each token names one slot of its own device. For each owner the named slots are the first ones of its 8 slots, every such slot is named by some token, and on every device some owner has all 8 slots named. Slots that no token names still ask for a row (each a distinct one); their gradient is zero. `seq_lengths`: the lengths of one device sum to 128; the longest is exactly 48.
All inputs are finite; a program needn't handle non-finite values.
Results may differ from the reference program's by a relative error of at most 0.014.
Values may be sent and summed in bfloat16 or wider, within the bound.
No kernel may reach another device: no remote copies, remote signals or barrier semaphores. Data moves between devices by JAX's collectives and lax.ppermute only.
A program may use at most 64 MiB of HBM per device.

```python
import math
import jax
import jax.numpy as jnp
import numpy as np
from jax import lax

E = 256
HEADS = 4
TOK_DEV = 128
SEQS = 8
MAXLEN = 48
ROWS_DEV = 1024
TOKENS = 2048
ROWS_TOTAL = 16384
N_SHARD = 16
N_REPLICA = 2


def device_plan(device_key):
    capacity = TOK_DEV // N_SHARD
    split_keys = jax.random.split(device_key, 6)
    counts = jax.random.randint(split_keys[0], (N_SHARD,), 1, capacity + 1)
    full_owner = jax.random.randint(split_keys[1], (), 0, N_SHARD)
    counts = jnp.where(jnp.arange(N_SHARD) == full_owner, capacity, counts)
    slot_index = jnp.arange(TOK_DEV, dtype=jnp.int32)
    owner_of = slot_index // capacity
    in_bucket = slot_index % capacity
    is_live = in_bucket < counts[owner_of]
    row_start = jax.random.randint(split_keys[2], (N_SHARD,), 0, ROWS_DEV)
    row_step = 2 * jax.random.randint(split_keys[3], (N_SHARD,), 0, ROWS_DEV // 2) + 1
    asked = ((row_start[owner_of] + row_step[owner_of] * in_bucket) % ROWS_DEV).astype(jnp.int32)
    live_first = jnp.argsort(1 - is_live.astype(jnp.int32), stable=True).astype(jnp.int32)
    live_count = jnp.sum(is_live.astype(jnp.int32))
    chosen = jax.random.randint(split_keys[4], (TOK_DEV,), 0, live_count)
    source_slot = jnp.where(slot_index < live_count, slot_index, chosen)
    token_slots = live_first[source_slot]
    shuffle = jax.random.permutation(split_keys[5], TOK_DEV)
    return (asked, token_slots[shuffle].astype(jnp.int32))


def slot_plan(key):
    device_keys = jax.random.split(jax.random.fold_in(key, 11), N_REPLICA * N_SHARD)
    asked, token_slots = jax.vmap(device_plan)(device_keys)
    return (asked, token_slots)


def draw_request_rows(key, part):
    asked, token_slots = slot_plan(key)
    return asked.reshape(N_REPLICA, N_SHARD, TOK_DEV)


def draw_token_slot(key, part):
    asked, token_slots = slot_plan(key)
    return token_slots.reshape(N_REPLICA, N_SHARD * TOK_DEV)


def levels(key, dims, cuts, smallest, largest):
    def one(position, parts):
        heights = jax.random.uniform(jax.random.fold_in(jax.random.fold_in(key, 6), position), (parts,), jnp.float32, smallest / len(cuts), largest / len(cuts))
        return jnp.repeat(jnp.exp(heights), dims[position] // parts).reshape((-1,) + (1,) * (len(dims) - position - 1))

    gain = one(*cuts[0])
    for cut in cuts[1:]:
        gain = gain * one(*cut)
    return gain


def profile(count, total, most, slope):
    portions = [(1 << 20) // math.isqrt(standing ** slope) + 1 for standing in range(2, count + 1)]
    rest, given = total - most - (count - 1), [1] * (count - 1)
    while rest > 0:
        movable = [i for i in range(count - 1) if given[i] < most]
        whole, left = sum([portions[i] for i in movable]), rest
        for i in movable:
            extra = min(most - given[i], max(1, left * portions[i] // whole), rest)
            given[i] = given[i] + extra
            rest = rest - extra
    return np.array([most] + given)


def ragged(stream_key, count, total, bound, skew):
    if count == 2:
        one = jax.random.randint(stream_key, (), max(1, total - bound), min(bound, total - 1) + 1)
        return jnp.stack([one, total - one])
    tallies = jnp.asarray(profile(count, total, bound, skew), jnp.int32)
    couples = (count - 1) // 2
    donor, sink = tallies[1:1 + 2 * couples:2], tallies[2:2 + 2 * couples:2]
    room = jnp.minimum(donor - 1, bound - sink)
    shifted = jax.random.randint(jax.random.fold_in(stream_key, 1), (couples,), 0, 1 << 20) % (room + 1)
    tallies = tallies.at[1:1 + 2 * couples:2].set(donor - shifted).at[2:2 + 2 * couples:2].set(sink + shifted)
    return tallies[jax.random.permutation(jax.random.fold_in(stream_key, 2), count)]


def gaussian(stream_key, extent, deviation, reach, cuts=(), held_as=jnp.bfloat16):
    gain = levels(stream_key, extent, cuts, -0.22, 0.18) if cuts else 1.0
    values = jax.random.normal(stream_key, extent, jnp.float32) * deviation * gain
    return jnp.minimum(jnp.maximum(values, -reach), reach).astype(held_as)


def setup_inputs(seed: int = 0) -> dict:
    key_list = jax.random.split(jax.random.key(seed), 11)
    request_rows = draw_request_rows(jax.random.fold_in(key_list[10], 71), 0)
    token_slot = draw_token_slot(jax.random.fold_in(key_list[10], 71), 0)
    seq_lengths = jax.vmap(lambda own: ragged(own, SEQS, TOK_DEV, MAXLEN, 2))(jax.random.split(key_list[2], N_REPLICA * N_SHARD)).reshape((N_REPLICA, N_SHARD, SEQS)).astype(jnp.int32)
    cotangent = gaussian(key_list[3], (N_REPLICA, TOKENS, E), 1.0, 6.0, ((0, 2), (1, 16)))
    table_slab = gaussian(key_list[4], (ROWS_TOTAL, E), 1.0, 6.0, ((0, 16),), jnp.float32)
    adagrad_state = jnp.clip(jnp.exp(math.log(1.0) - 2.3025851 * jax.random.uniform(key_list[5], (ROWS_TOTAL,), jnp.float32) ** levels(key_list[5], (ROWS_TOTAL,), ((0, 16),), -0.2, 0.2)), 0.1, 1.0)
    w_uvqk = gaussian(key_list[6], (E, 4 * E), E ** -0.5, 0.375)
    w_out = gaussian(key_list[7], (E, E), E ** -0.5, 0.375)
    norm_gain = jnp.clip(1.0 + 0.18 * jax.random.normal(key_list[8], (E,), jnp.float32), 0.1, 1.9)
    out_gain = jnp.clip(1.0 + 0.18 * jax.random.normal(key_list[9], (E,), jnp.float32), 0.1, 1.9)
    return {"request_rows": request_rows, "token_slot": token_slot, "seq_lengths": seq_lengths, "cotangent": cotangent, "table_slab": table_slab, "adagrad_state": adagrad_state, "w_uvqk": w_uvqk, "w_out": w_out, "norm_gain": norm_gain, "out_gain": out_gain}


epsilon = 1e-08
learn_rate = 0.5

def normalize(values):
    center = values - lax.optimization_barrier(jnp.mean(values, axis=1, keepdims=True))
    variance = lax.optimization_barrier(jnp.mean(center * center, axis=1, keepdims=True))
    return center * lax.rsqrt(variance + 1e-05)

def same_sequence(lengths, count):
    seq_ends = jnp.cumsum(lengths)
    positions = jnp.arange(count, dtype=jnp.int32)
    segment = lax.optimization_barrier(jnp.sum(positions[:, None] >= seq_ends[None, :], axis=1))
    return (segment[:, None] == segment[None, :]) & (positions[:, None] >= positions[None, :])

def hstu_layer(embedded, w_uvqk, w_out, norm_gain, out_gain, same_seq):
    count = embedded.shape[0]
    model_width = embedded.shape[1]
    head_width = model_width // HEADS
    normed = (normalize(embedded) * norm_gain).astype(jnp.bfloat16)
    projected = jax.nn.silu(jnp.dot(normed, w_uvqk, preferred_element_type=jnp.float32))
    gate_u = projected[:, :model_width]
    packed = projected[:, model_width:].astype(jnp.bfloat16).reshape(count, 3, HEADS, head_width)
    values = packed[:, 0].astype(jnp.float32)
    queries = packed[:, 1].astype(jnp.float32)
    key_rows = packed[:, 2].astype(jnp.float32)
    scores = jnp.einsum('qhd,khd->hqk', queries, key_rows) * head_width ** (-0.5)
    weights = jnp.where(same_seq[None], jax.nn.silu(scores) / MAXLEN, 0.0).astype(jnp.bfloat16)
    attended = jnp.einsum('hqk,khd->qhd', weights.astype(jnp.float32), values).reshape(count, model_width)
    gated = (normalize(attended) * out_gain * gate_u).astype(jnp.bfloat16)
    return embedded + jnp.dot(gated, w_out, preferred_element_type=jnp.float32)

def reference(request_rows, token_slot, seq_lengths, cotangent, table_slab, adagrad_state, w_uvqk, w_out, norm_gain, out_gain):
    capacity = TOK_DEV // N_SHARD
    owners = jnp.arange(TOK_DEV, dtype=jnp.int32) // capacity * ROWS_DEV
    slot_all = token_slot.reshape(N_REPLICA, N_SHARD, TOK_DEV)
    cotan_all = cotangent.reshape(N_REPLICA, N_SHARD, TOK_DEV, E)
    grad_scale = 1.0 / math.sqrt(TOK_DEV * N_SHARD * N_REPLICA)

    def device_step(state_carry, device_item):
        row_grads, dense_sums = state_carry
        asked_rows, slot_ids, lengths, cotan_rows = device_item
        flat_rows = owners + asked_rows.astype(jnp.int32)
        found_rows = table_slab[flat_rows].astype(jnp.bfloat16)
        embedded = found_rows[slot_ids].astype(jnp.float32)
        same_seq = same_sequence(lengths, TOK_DEV)

        def local_layer(first, second, third, fourth, fifth):
            return hstu_layer(first, second, third, fourth, fifth, same_seq)
        unused, pullback = jax.vjp(local_layer, embedded, w_uvqk, w_out, norm_gain, out_gain)
        token_grad, grad_one, grad_two, grad_norm, grad_gate = pullback(cotan_rows.astype(jnp.float32))
        slot_grad = jax.ops.segment_sum(token_grad, slot_ids, num_segments=TOK_DEV)
        row_grads = row_grads.at[flat_rows].add(slot_grad)
        dense_sums = (dense_sums[0] + grad_one.astype(jnp.float32) * grad_scale, dense_sums[1] + grad_two.astype(jnp.float32) * grad_scale, dense_sums[2] + jnp.stack([grad_norm, grad_gate]).astype(jnp.float32) * grad_scale)
        return ((row_grads, dense_sums), None)

    def replica_step(state_carry, replica_item):
        delta_sum, square_sum, dense_sums = state_carry
        initial = (jnp.zeros((ROWS_TOTAL, E), jnp.float32), dense_sums)
        (row_grads, dense_sums), unused = lax.scan(device_step, initial, replica_item)
        mean_square = lax.optimization_barrier(jnp.mean(row_grads * row_grads, axis=1))
        row_delta = -learn_rate * row_grads / jnp.sqrt(adagrad_state + mean_square + epsilon)[:, None]
        return ((delta_sum + row_delta, square_sum + mean_square, dense_sums), None)
    initial = (jnp.zeros((ROWS_TOTAL, E), jnp.float32), jnp.zeros((ROWS_TOTAL,), jnp.float32), (jnp.zeros((E, 4 * E), jnp.float32), jnp.zeros((E, E), jnp.float32), jnp.zeros((2, E), jnp.float32)))
    (delta_sum, square_sum, dense_sums), unused = lax.scan(replica_step, initial, (request_rows, slot_all, seq_lengths, cotan_all))
    return (delta_sum / N_REPLICA, adagrad_state + square_sum / N_REPLICA, dense_sums[0], dense_sums[1], dense_sums[2])
```

```python
import functools
import math

import jax
import jax.numpy as jnp
from jax import lax
from jax.experimental import pallas as pl
from jax.experimental.pallas import tpu as pltpu
from jax.sharding import PartitionSpec as P

HEADS = 4
MAXLEN = 48
EPSILON = 1e-08
LEARN_RATE = 0.5
NORM_EPSILON = 1e-05
GAIN_ROWS = 8

f32 = jnp.float32
bf16 = jnp.bfloat16
VMEM = pl.BlockSpec(memory_space=pltpu.VMEM)


def iota(shape, axis):
    return lax.broadcasted_iota(jnp.int32, shape, axis)


def mm(left, right, contract=(1, 0)):
    return lax.dot_general(
        left.astype(bf16),
        right.astype(bf16),
        (((contract[0],), (contract[1],)), ((), ())),
        preferred_element_type=f32,
    )


def estimate(flops, bytes_accessed):
    return pl.CostEstimate(flops=flops, bytes_accessed=bytes_accessed, transcendentals=0)


def fetch_kernel(capacity, ids_ref, table_ref, found_ref, wanted_ref):
    me = lax.axis_index("shard")
    ids = ids_ref[...].reshape(ids_ref.shape[0], ids_ref.shape[2])
    shards, slots = ids.shape
    rows = table_ref.shape[0]
    high = (ids >> 5).astype(f32)
    low = (ids & 31).astype(f32)
    slot = iota((slots, shards), 0)
    first = iota((slots, shards), 1) * capacity
    expand = ((slot >= first) & (slot < first + capacity)).astype(f32)
    asked = mm(expand, high) * 32.0 + mm(expand, low)
    pick = iota((slots, slots), 1) == me * capacity + lax.rem(iota((slots, slots), 0), capacity)
    column = jnp.sum(jnp.where(pick, asked, 0.0), axis=1, keepdims=True)
    eye = iota((slots, slots), 0) == iota((slots, slots), 1)
    wanted_ref[...] = jnp.sum(jnp.where(eye, column, 0.0), axis=0, keepdims=True)
    chosen = (column.astype(jnp.int32) == iota((slots, rows), 1)).astype(f32)
    found_ref[...] = mm(chosen, table_ref[...]).astype(bf16)


def center(values):
    shifted = values - jnp.mean(values, axis=1, keepdims=True)
    scale = lax.rsqrt(jnp.mean(shifted * shifted, axis=1, keepdims=True) + NORM_EPSILON)
    return shifted * scale, scale


def center_grad(grad, normal, scale):
    along = jnp.mean(grad * normal, axis=1, keepdims=True)
    return scale * (grad - jnp.mean(grad, axis=1, keepdims=True) - normal * along)


def sigmoid(values):
    return 1.0 / (1.0 + jnp.exp(-values))


def segments(lengths):
    count = lengths.shape[1]
    row, col = iota((count, count), 0), iota((count, count), 1)
    column = jnp.sum(jnp.where(row == col, lengths, 0.0), axis=1, keepdims=True)
    ends_column = jnp.sum(jnp.where(col <= row, lengths, 0.0), axis=1, keepdims=True)
    ends_row = jnp.sum(jnp.where(row <= col, column, 0.0), axis=0, keepdims=True)
    return ends_row, ends_column


def layer_kernel(
    slot_ref, rows_ref, length_ref, cot_ref, w_ref, wo_ref, norm_ref, gate_ref, slot_grad_ref, *rest
):
    part_refs, stacked = rest[:-1], rest[-1]
    replicas = len(part_refs)
    tokens, width = rows_ref.shape
    head = width // HEADS
    part_rows = part_refs[0].shape[0] - GAIN_ROWS
    row, col = iota((tokens, tokens), 0), iota((tokens, tokens), 1)

    slot_row = slot_ref[...].astype(f32)
    slot_column = jnp.sum(jnp.where(row == col, slot_row, 0.0), axis=1, keepdims=True)
    embedded = mm((slot_column.astype(jnp.int32) == col).astype(f32), rows_ref[...])

    ends_row, ends_column = segments(length_ref[...].astype(f32))
    count = ends_row.shape[1]
    before_row = iota((count, tokens), 1).astype(f32) >= ends_column
    segment_row = jnp.sum(before_row.astype(f32), axis=0, keepdims=True)
    before_column = iota((tokens, count), 0).astype(f32) >= ends_row
    segment_column = jnp.sum(before_column.astype(f32), axis=1, keepdims=True)
    same = (segment_row == segment_column) & (row >= col)
    same = jnp.concatenate([same.astype(f32)] * HEADS, axis=0)

    lane = iota((1, width), 1)
    heads = [((lane >= h * head) & (lane < (h + 1) * head)).astype(f32) for h in range(HEADS)]

    def by_head(values):
        return jnp.concatenate([values * mask for mask in heads], axis=0).astype(bf16)

    def beside(values):
        return jnp.concatenate(
            [values[h * tokens : (h + 1) * tokens] for h in range(HEADS)], axis=1
        )

    norm_gain, gate_gain = norm_ref[...], gate_ref[...]
    normal, scale = center(embedded)
    normed = (normal * norm_gain).astype(bf16)
    lifted = mm(normed, w_ref[...])
    sig = sigmoid(lifted)
    projected = lifted * sig
    slope = sig * (1.0 + lifted * (1.0 - sig))
    gate_u = projected[:, :width]
    values = projected[:, width : 2 * width].astype(bf16).astype(f32)
    queries = projected[:, 2 * width : 3 * width].astype(bf16).astype(f32)
    keys = projected[:, 3 * width :].astype(bf16).astype(f32)

    queries_by, keys_by, values_by = by_head(queries), by_head(keys), by_head(values)
    scores = mm(queries_by, keys, (1, 1)) * head ** (-0.5)
    score_sig = sigmoid(scores)
    weights = (same * (scores * score_sig / MAXLEN)).astype(bf16)
    attended = mm(beside(weights), values_by)
    normal_two, scale_two = center(attended)
    gated = (normal_two * gate_gain * gate_u).astype(bf16)

    cot = cot_ref[...]
    gated_grad = mm(cot, wo_ref[...], (1, 1)).astype(bf16).astype(f32)
    out_grad = mm(gated, cot, (0, 0))
    normal_u = normal_two * gate_u
    gate_gain_grad = jnp.sum(gated_grad * normal_u, axis=0, keepdims=True)
    gated_gain = gated_grad * gate_gain
    u_grad = gated_gain * normal_two
    attended_grad = center_grad(gated_gain * gate_u, normal_two, scale_two)
    attended_by = by_head(attended_grad)
    weights_grad = mm(attended_by, values, (1, 1)).astype(bf16).astype(f32)
    values_grad = mm(weights, attended_by, (0, 0)).astype(bf16).astype(f32)
    score_slope = score_sig * (1.0 + scores * (1.0 - score_sig))
    scores_grad = (same * weights_grad * score_slope * (head ** (-0.5) / MAXLEN)).astype(bf16)
    queries_grad = mm(beside(scores_grad), keys_by).astype(bf16).astype(f32)
    keys_grad = mm(scores_grad, queries_by, (0, 0)).astype(bf16).astype(f32)
    lifted_grad = (
        jnp.concatenate([u_grad, values_grad, queries_grad, keys_grad], axis=1) * slope
    ).astype(bf16)
    w_grad = mm(normed, lifted_grad, (0, 0)).astype(bf16)
    normed_grad = mm(lifted_grad, w_ref[...], (1, 1)).astype(bf16).astype(f32)
    norm_gain_grad = jnp.sum(normed_grad * normal, axis=0, keepdims=True)
    token_grad = cot.astype(f32) + center_grad(normed_grad * norm_gain, normal, scale)

    to_slot = (slot_row.astype(jnp.int32) == row).astype(f32)
    grad_high = token_grad.astype(bf16).astype(f32)
    slot_grad_ref[...] = mm(
        jnp.concatenate([to_slot, to_slot], axis=1),
        jnp.concatenate([grad_high, token_grad - grad_high], axis=0),
    ).astype(bf16)

    blocks = w_grad.shape[1] // width
    for block in range(blocks):
        stacked[block * width : (block + 1) * width] = w_grad[:, block * width : (block + 1) * width]
    stacked[blocks * width : (blocks + 1) * width] = out_grad.astype(bf16)
    filled = (blocks + 1) * width
    if filled < stacked.shape[0]:
        stacked[filled:] = jnp.zeros((stacked.shape[0] - filled, width), bf16)
    gain_grads = jnp.concatenate([norm_gain_grad, gate_gain_grad], axis=0)
    gain_high = gain_grads.astype(bf16).astype(f32)
    gain_rows = jnp.concatenate(
        [gain_high, gain_grads - gain_high, jnp.zeros((GAIN_ROWS - 4, width), f32)], axis=0
    ).astype(bf16)
    me = lax.axis_index("replica")
    for step, part_ref in enumerate(part_refs):
        start = lax.rem(me + step, replicas) * part_rows
        part_ref[:part_rows] = stacked[pl.ds(pl.multiple_of(start, 16), part_rows)]
        part_ref[part_rows:] = gain_rows


def pack_kernel(shards, slot_grad_ref, *refs):
    part_refs, out_ref = refs[:-1], refs[-1]
    width = slot_grad_ref.shape[1]
    total = part_refs[0][...].astype(f32)
    for part_ref in part_refs[1:]:
        total = total + part_ref[...].astype(f32)
    share = total[:-GAIN_ROWS].reshape(shards, -1, width)
    gains = jnp.broadcast_to(total[-GAIN_ROWS:][None], (shards, GAIN_ROWS, width))
    slots = slot_grad_ref[...].astype(f32).reshape(shards, -1, width)
    out_ref[...] = jnp.concatenate([slots, share, gains], axis=1).astype(bf16)


def unpack_kernel(capacity, grad_scale, in_ref, slots_ref, share_ref, gains_ref):
    shards, rows, width = in_ref.shape
    slots_ref[...] = in_ref[:, :capacity].astype(f32).reshape(-1, width).astype(bf16)
    total = in_ref[0, capacity:].astype(f32)
    for shard in range(1, shards):
        total = total + in_ref[shard, capacity:].astype(f32)
    total = total * grad_scale
    share = total[:-GAIN_ROWS].astype(bf16)
    for shard in range(shards):
        share_ref[shard] = share
    first = total.shape[0] - GAIN_ROWS
    gains_ref[...] = total[first : first + 2] + total[first + 2 : first + 4]


def adagrad_kernel(replicas, *refs):
    wanted_refs, grad_refs = refs[:replicas], refs[replicas : 2 * replicas]
    state_ref, update_ref, state_out_ref = refs[2 * replicas :]
    rows = update_ref.shape[0]
    slots = wanted_refs[0].shape[1]
    first = pl.program_id(0) * rows
    eye = iota((rows, rows), 0) == iota((rows, rows), 1)
    state_row = state_ref[...].reshape(1, rows)
    state = jnp.sum(jnp.where(eye, state_row, 0.0), axis=1, keepdims=True)
    delta = jnp.zeros(update_ref.shape, f32)
    squares = jnp.zeros((rows, 1), f32)
    for wanted_ref, grad_ref in zip(wanted_refs, grad_refs):
        hit = iota((rows, slots), 0) + first == wanted_ref[...].astype(jnp.int32)
        row_grad = mm(hit.astype(f32), grad_ref[...])
        mean_square = jnp.mean(row_grad * row_grad, axis=1, keepdims=True)
        delta = delta + row_grad * lax.rsqrt(state + mean_square + EPSILON)
        squares = squares + mean_square
    update_ref[...] = delta * (-LEARN_RATE / replicas)
    squares_row = jnp.sum(jnp.where(eye, squares, 0.0), axis=0, keepdims=True)
    state_out_ref[...] = (state_row + squares_row / replicas).reshape(state_out_ref.shape)


def spread_kernel(ordered, *refs):
    part_refs, (uvqk_ref, out_ref) = refs[:-2], refs[-2:]
    parts = [part_ref[...] for part_ref in part_refs]
    if not ordered:
        mine, other = parts
        is_first = lax.axis_index("replica") == 0
        parts = [jnp.where(is_first, mine, other), jnp.where(is_first, other, mine)]
    width = parts[0].shape[1]
    rows = jnp.concatenate(parts, axis=0).astype(f32)
    blocks = uvqk_ref.shape[1] // width
    for block in range(blocks):
        uvqk_ref[:, block * width : (block + 1) * width] = rows[block * width : (block + 1) * width]
    out_ref[...] = rows[blocks * width : (blocks + 1) * width]


def from_replicas(parts):
    replicas = len(parts)
    came = [parts[0]]
    for step in range(1, replicas):
        pairs = [(source, (source + step) % replicas) for source in range(replicas)]
        came.append(lax.ppermute(parts[step], "replica", pairs))
    if replicas > 2:
        order = lax.rem(lax.axis_index("replica") - jnp.arange(replicas) + replicas, replicas)
        stacked = jnp.take(jnp.stack(came), order, axis=0)
        came = [stacked[index] for index in range(replicas)]
    return came


def on_device(
    request_rows,
    token_slot,
    seq_lengths,
    cotangent,
    table_slab,
    adagrad_state,
    w_uvqk,
    w_out,
    norm_gain,
    out_gain,
):
    shards = lax.axis_size("shard")
    replicas = lax.axis_size("replica")
    tokens = token_slot.shape[1]
    rows_dev, width = table_slab.shape
    capacity = tokens // shards
    dense_rows = w_uvqk.shape[1] + width
    share_rows = -(-dense_rows // (shards * replicas))
    part_rows = share_rows * shards
    grad_scale = 1.0 / math.sqrt(tokens * shards * replicas)
    shape = jax.ShapeDtypeStruct

    asked = jnp.broadcast_to(request_rows.reshape(1, 1, tokens), (shards, 1, tokens))
    ids = lax.all_to_all(asked, "shard", split_axis=0, concat_axis=0, tiled=True)
    found, wanted = pl.pallas_call(
        functools.partial(fetch_kernel, capacity),
        out_shape=(shape((tokens, width), bf16), shape((1, tokens), f32)),
        in_specs=[VMEM] * 2,
        out_specs=(VMEM, VMEM),
        cost_estimate=estimate(2 * tokens * rows_dev * width, rows_dev * width * 4),
        name="fetch",
    )(ids, table_slab)
    slot_rows = lax.all_to_all(
        found.reshape(shards, capacity, width), "shard", split_axis=0, concat_axis=0, tiled=True
    ).reshape(tokens, width)

    part_shape = shape((part_rows + GAIN_ROWS, width), bf16)
    slot_grad, *parts = pl.pallas_call(
        layer_kernel,
        out_shape=(shape((tokens, width), bf16),) + (part_shape,) * replicas,
        in_specs=[VMEM] * 8,
        out_specs=(VMEM,) * (replicas + 1),
        scratch_shapes=[pltpu.VMEM((part_rows * replicas, width), bf16)],
        cost_estimate=estimate(8 * tokens * width * w_uvqk.shape[1], 4 * dense_rows * width),
        name="layer",
    )(
        token_slot,
        slot_rows,
        seq_lengths.reshape(1, -1),
        cotangent.reshape(tokens, width),
        w_uvqk,
        w_out,
        norm_gain.reshape(1, width),
        out_gain.reshape(1, width),
    )

    came = from_replicas(parts)
    aligned = capacity % 8 == 0 and share_rows % 8 == 0
    message_rows = capacity + share_rows + GAIN_ROWS
    if aligned:
        message = pl.pallas_call(
            functools.partial(pack_kernel, shards),
            out_shape=shape((shards, message_rows, width), bf16),
            in_specs=[VMEM] * (replicas + 1),
            out_specs=VMEM,
            name="pack",
        )(slot_grad, *came)
    else:
        total = sum(part.astype(f32) for part in came).astype(bf16)
        message = jnp.concatenate(
            [
                slot_grad.reshape(shards, capacity, width),
                total[:part_rows].reshape(shards, share_rows, width),
                jnp.broadcast_to(total[part_rows:][None], (shards, GAIN_ROWS, width)),
            ],
            axis=1,
        )
    arrived = lax.all_to_all(message, "shard", split_axis=0, concat_axis=0, tiled=True)
    if aligned:
        owned, share, grad_gains = pl.pallas_call(
            functools.partial(unpack_kernel, capacity, grad_scale),
            out_shape=(
                shape((tokens, width), bf16),
                shape((shards, share_rows, width), bf16),
                shape((2, width), f32),
            ),
            in_specs=[VMEM],
            out_specs=(VMEM,) * 3,
            name="unpack",
        )(arrived)
    else:
        owned = arrived[:, :capacity].reshape(tokens, width)
        total = jnp.sum(arrived[:, capacity:].astype(f32), axis=0) * grad_scale
        share = jnp.broadcast_to(
            total[:share_rows].astype(bf16)[None], (shards, share_rows, width)
        )
        grad_gains = total[share_rows : share_rows + 2] + total[share_rows + 2 : share_rows + 4]

    gathered = lax.all_to_all(share, "shard", split_axis=0, concat_axis=0, tiled=True)

    wanted_all = from_replicas([wanted] * replicas)
    owned_all = from_replicas([owned] * replicas)
    block = 128
    row_update, state_new = pl.pallas_call(
        functools.partial(adagrad_kernel, replicas),
        grid=(rows_dev // block,),
        out_shape=(shape((rows_dev, width), f32), shape((rows_dev // block, 1, block), f32)),
        in_specs=[pl.BlockSpec((1, tokens), lambda step: (0, 0))] * replicas
        + [pl.BlockSpec((tokens, width), lambda step: (0, 0))] * replicas
        + [pl.BlockSpec((1, 1, block), lambda step: (step, 0, 0))],
        out_specs=(
            pl.BlockSpec((block, width), lambda step: (step, 0)),
            pl.BlockSpec((1, 1, block), lambda step: (step, 0, 0)),
        ),
        cost_estimate=estimate(2 * replicas * tokens * rows_dev * width, rows_dev * width * 4),
        name="adagrad",
    )(*wanted_all, *owned_all, adagrad_state.reshape(rows_dev // block, 1, block))

    halves = from_replicas([gathered.reshape(part_rows, width)] * replicas)
    grad_uvqk, grad_out = pl.pallas_call(
        functools.partial(spread_kernel, replicas != 2),
        out_shape=(shape(w_uvqk.shape, f32), shape(w_out.shape, f32)),
        in_specs=[VMEM] * replicas,
        out_specs=(VMEM, VMEM),
        name="spread",
    )(*halves)
    return (row_update, state_new.reshape(rows_dev), grad_uvqk, grad_out, grad_gains)


def solution(mesh):
    placed = (
        P("replica", "shard", None),
        P("replica", "shard"),
        P("replica", "shard", None),
        P("replica", "shard", None),
        P("shard", None),
        P("shard"),
        P(),
        P(),
        P(),
        P(),
    )
    return jax.shard_map(
        on_device,
        mesh=mesh,
        in_specs=placed,
        out_specs=(P("shard", None), P("shard"), P(), P(), P()),
        check_vma=False,
    )
```

```python
import functools
import math

import jax
import jax.numpy as jnp
from jax import lax
from jax.experimental import pallas as pl
from jax.experimental.pallas import tpu as pltpu
from jax.sharding import PartitionSpec as P


HEADS = 4
MAXLEN = 48
EPSILON = 1e-08
LEARN_RATE = 0.5
NORM_EPSILON = 1e-05
GAIN_ROWS = 8

f32 = jnp.float32
bf16 = jnp.bfloat16
VMEM = pl.BlockSpec(memory_space=pltpu.VMEM)


def room(mebibytes):
    return pltpu.CompilerParams(vmem_limit_bytes=mebibytes * 2**20)


def iota(shape, axis):
    return lax.broadcasted_iota(jnp.int32, shape, axis)


def mm(left, right, contract=(1, 0)):
    return lax.dot_general(
        left.astype(bf16),
        right.astype(bf16),
        (((contract[0],), (contract[1],)), ((), ())),
        preferred_element_type=f32,
    )


def estimate(flops, bytes_accessed):
    return pl.CostEstimate(flops=flops, bytes_accessed=bytes_accessed, transcendentals=0)


def ready_kernel(asked_ref, slot_ref, length_ref, norm_ref, gate_ref, ids_ref, small_ref):
    ids_ref[...] = jnp.broadcast_to(asked_ref[...], ids_ref.shape)
    small_ref[0:1, : slot_ref.shape[1]] = slot_ref[...].astype(f32)
    small_ref[1:2, : length_ref.shape[1]] = length_ref[...].astype(f32)
    small_ref[2:3, : norm_ref.shape[1]] = norm_ref[...]
    small_ref[3:4, : gate_ref.shape[1]] = gate_ref[...]


def fetch_kernel(capacity, ids_ref, table_ref, found_ref, wanted_ref):
    me = lax.axis_index("shard")
    ids = ids_ref[...].reshape(ids_ref.shape[0], ids_ref.shape[2])
    shards, slots = ids.shape
    rows = table_ref.shape[0]
    high = (ids >> 5).astype(f32)
    low = (ids & 31).astype(f32)
    slot = iota((slots, shards), 0)
    first = iota((slots, shards), 1) * capacity
    expand = ((slot >= first) & (slot < first + capacity)).astype(f32)
    asked = mm(expand, high) * 32.0 + mm(expand, low)
    pick = iota((slots, slots), 1) == me * capacity + lax.rem(iota((slots, slots), 0), capacity)
    column = jnp.sum(jnp.where(pick, asked, 0.0), axis=1, keepdims=True)
    eye = iota((slots, slots), 0) == iota((slots, slots), 1)
    wanted_ref[...] = jnp.sum(jnp.where(eye, column, 0.0), axis=0, keepdims=True)
    chosen = (column.astype(jnp.int32) == iota((slots, rows), 1)).astype(f32)
    found_ref[...] = mm(chosen, table_ref[...]).astype(bf16)


def center(values):
    shifted = values - jnp.mean(values, axis=1, keepdims=True)
    scale = lax.rsqrt(jnp.mean(shifted * shifted, axis=1, keepdims=True) + NORM_EPSILON)
    return shifted * scale, scale


def center_grad(grad, normal, scale):
    along = jnp.mean(grad * normal, axis=1, keepdims=True)
    return scale * (grad - jnp.mean(grad, axis=1, keepdims=True) - normal * along)


def sigmoid(values):
    return 1.0 / (1.0 + jnp.exp(-values))


def segments(lengths):
    count = lengths.shape[1]
    row, col = iota((count, count), 0), iota((count, count), 1)
    column = jnp.sum(jnp.where(row == col, lengths, 0.0), axis=1, keepdims=True)
    ends_column = jnp.sum(jnp.where(col <= row, lengths, 0.0), axis=1, keepdims=True)
    ends_row = jnp.sum(jnp.where(row <= col, column, 0.0), axis=0, keepdims=True)
    return ends_row, ends_column


def layer_kernel(
    histories, small_ref, rows_ref, cot_ref, w_ref, wo_ref, lifted_ref, normal_ref, gate_ref, *rest
):
    part_refs, stacked = rest[:-1], rest[-1]
    replicas = len(part_refs)
    tokens, width = rows_ref.shape
    head = width // HEADS
    row, col = iota((tokens, tokens), 0), iota((tokens, tokens), 1)

    slot_row = small_ref[0:1, :tokens]
    slot_column = jnp.sum(jnp.where(row == col, slot_row, 0.0), axis=1, keepdims=True)
    embedded = mm((slot_column.astype(jnp.int32) == col).astype(f32), rows_ref[...])

    ends_row, ends_column = segments(small_ref[1:2, :histories])
    before_row = iota((histories, tokens), 1).astype(f32) >= ends_column
    segment_row = jnp.sum(before_row.astype(f32), axis=0, keepdims=True)
    before_column = iota((tokens, histories), 0).astype(f32) >= ends_row
    segment_column = jnp.sum(before_column.astype(f32), axis=1, keepdims=True)
    same = (segment_row == segment_column) & (row >= col)
    same = jnp.concatenate([same.astype(f32)] * HEADS, axis=0)

    lane = iota((1, width), 1)
    heads = [((lane >= h * head) & (lane < (h + 1) * head)).astype(f32) for h in range(HEADS)]

    def by_head(values):
        return jnp.concatenate([values * mask for mask in heads], axis=0).astype(bf16)

    def beside(values):
        return jnp.concatenate(
            [values[h * tokens : (h + 1) * tokens] for h in range(HEADS)], axis=1
        )

    norm_gain, gate_gain = small_ref[2:3, :width], small_ref[3:4, :width]
    normal, scale = center(embedded)
    normed = (normal * norm_gain).astype(bf16)
    lifted = mm(normed, w_ref[...])
    sig = sigmoid(lifted)
    projected = lifted * sig
    slope = sig * (1.0 + lifted * (1.0 - sig))
    gate_u = projected[:, :width]
    values = projected[:, width : 2 * width].astype(bf16).astype(f32)
    queries = projected[:, 2 * width : 3 * width].astype(bf16).astype(f32)
    keys = projected[:, 3 * width :].astype(bf16).astype(f32)

    queries_by, keys_by, values_by = by_head(queries), by_head(keys), by_head(values)
    scores = mm(queries_by, keys, (1, 1)) * head ** (-0.5)
    score_sig = sigmoid(scores)
    weights = (same * (scores * score_sig / MAXLEN)).astype(bf16)
    attended = mm(beside(weights), values_by)
    normal_two, scale_two = center(attended)
    gated = (normal_two * gate_gain * gate_u).astype(bf16)

    cot = cot_ref[...]
    gated_grad = mm(cot, wo_ref[...], (1, 1)).astype(bf16).astype(f32)
    out_grad = mm(gated, cot, (0, 0))
    normal_u = normal_two * gate_u
    gate_ref[...] = jnp.sum(gated_grad * normal_u, axis=0, keepdims=True)
    gated_gain = gated_grad * gate_gain
    u_grad = gated_gain * normal_two
    attended_grad = center_grad(gated_gain * gate_u, normal_two, scale_two)
    attended_by = by_head(attended_grad)
    weights_grad = mm(attended_by, values, (1, 1)).astype(bf16).astype(f32)
    values_grad = mm(weights, attended_by, (0, 0)).astype(bf16).astype(f32)
    score_slope = score_sig * (1.0 + scores * (1.0 - score_sig))
    scores_grad = (same * weights_grad * score_slope * (head ** (-0.5) / MAXLEN)).astype(bf16)
    queries_grad = mm(beside(scores_grad), keys_by).astype(bf16).astype(f32)
    keys_grad = mm(scores_grad, queries_by, (0, 0)).astype(bf16).astype(f32)
    lifted_grad = (
        jnp.concatenate([u_grad, values_grad, queries_grad, keys_grad], axis=1) * slope
    ).astype(bf16)
    lifted_ref[...] = lifted_grad
    normal_ref[:, :width] = normal
    normal_ref[:, width:] = jnp.broadcast_to(scale, (tokens, normal_ref.shape[1] - width))
    w_grad = mm(normed, lifted_grad, (0, 0)).astype(bf16)

    blocks = w_grad.shape[1] // width
    for block in range(blocks):
        stacked[block * width : (block + 1) * width] = w_grad[:, block * width : (block + 1) * width]
    stacked[blocks * width :] = out_grad.astype(bf16)
    me = lax.axis_index("replica")
    height = width // replicas
    for step, part_ref in enumerate(part_refs):
        start = lax.rem(me + step, replicas) * height
        for block in range(blocks + 1):
            part_ref[block * height : (block + 1) * height] = stacked[
                pl.ds(pl.multiple_of(block * width + start, 16), height)
            ]
        filled = (blocks + 1) * height
        if filled < part_ref.shape[0]:
            part_ref[filled:] = jnp.zeros((part_ref.shape[0] - filled, width), bf16)


def finish_kernel(small_ref, cot_ref, w_ref, lifted_ref, normal_ref, gate_ref, slot_grad_ref, gain_ref):
    tokens, width = cot_ref.shape
    normal = normal_ref[:, :width]
    scale = normal_ref[:, width : width + 1]
    normed_grad = mm(lifted_ref[...], w_ref[...], (1, 1)).astype(bf16).astype(f32)
    norm_gain_grad = jnp.sum(normed_grad * normal, axis=0, keepdims=True)
    token_grad = cot_ref[...].astype(f32) + center_grad(
        normed_grad * small_ref[2:3, :width], normal, scale
    )
    slot_row = small_ref[0:1, :tokens].astype(jnp.int32)
    to_slot = (slot_row == iota((tokens, tokens), 0)).astype(f32)
    grad_high = token_grad.astype(bf16).astype(f32)
    slot_grad_ref[...] = mm(
        jnp.concatenate([to_slot, to_slot], axis=1),
        jnp.concatenate([grad_high, token_grad - grad_high], axis=0),
    ).astype(bf16)
    gains = jnp.concatenate([norm_gain_grad, gate_ref[...]], axis=0)
    high = gains.astype(bf16).astype(f32)
    gain_ref[...] = jnp.concatenate([high, gains - high], axis=0)


def halves_down(values):
    lanes = values.shape[-1] // 2
    return jnp.concatenate([values[..., :lanes], values[..., lanes:]], axis=-2)


def halves_across(values):
    rows = values.shape[-2] // 2
    return jnp.concatenate([values[..., :rows, :], values[..., rows:, :]], axis=-1)


def pack_kernel(shards, slot_grad_ref, gain_ref, *refs):
    part_refs, out_ref = refs[:-1], refs[-1]
    width = slot_grad_ref.shape[1]
    total = part_refs[0][...].astype(f32)
    for part_ref in part_refs[1:]:
        total = total + part_ref[...].astype(f32)
    share = total.reshape(shards, -1, width)
    gains = halves_down(gain_ref[...])
    gains = jnp.broadcast_to(gains[None], (shards,) + gains.shape)
    slots = slot_grad_ref[...].astype(f32).reshape(shards, -1, width)
    out_ref[...] = jnp.concatenate(
        [halves_down(slots), halves_down(share), gains], axis=1
    ).astype(bf16)


def unpack_kernel(capacity, grad_scale, in_ref, share_ref):
    shards, rows, _ = in_ref.shape
    wanted = slice(2 * capacity, rows - GAIN_ROWS)
    total = in_ref[0, wanted].astype(f32)
    for shard in range(1, shards):
        total = total + in_ref[shard, wanted].astype(f32)
    share = halves_across(total * grad_scale).astype(bf16)
    for shard in range(shards):
        share_ref[shard] = share


def slots_kernel(capacity, grad_scale, in_ref, slots_ref):
    shards, rows, lanes = in_ref.shape
    tokens = shards * capacity
    slots = halves_across(in_ref[:, : 2 * capacity].astype(f32))
    gains = halves_across(jnp.sum(in_ref[:, rows - GAIN_ROWS :].astype(f32), axis=0))
    gains = (gains[:2] + gains[2:]) * grad_scale
    high = gains.astype(bf16).astype(f32)
    padding = jnp.zeros((slots_ref.shape[0] - tokens - 4, 2 * lanes), f32)
    slots_ref[...] = jnp.concatenate(
        [slots.reshape(tokens, 2 * lanes), high, gains - high, padding], axis=0
    ).astype(bf16)


def adagrad_kernel(replicas, *refs):
    wanted_refs, grad_refs = refs[:replicas], refs[replicas : 2 * replicas]
    state_ref, update_ref, state_out_ref, gains_ref = refs[2 * replicas :]
    rows = update_ref.shape[0]
    slots = wanted_refs[0].shape[1]
    first = pl.program_id(0) * rows
    eye = iota((rows, rows), 0) == iota((rows, rows), 1)
    state_row = state_ref[...].reshape(1, rows)
    state = jnp.sum(jnp.where(eye, state_row, 0.0), axis=1, keepdims=True)
    delta = jnp.zeros(update_ref.shape, f32)
    squares = jnp.zeros((rows, 1), f32)
    gains = jnp.zeros((grad_refs[0].shape[0] - slots, update_ref.shape[1]), f32)
    for wanted_ref, grad_ref in zip(wanted_refs, grad_refs):
        hit = iota((rows, slots), 0) + first == wanted_ref[...].astype(jnp.int32)
        row_grad = mm(hit.astype(f32), grad_ref[:slots])
        mean_square = jnp.mean(row_grad * row_grad, axis=1, keepdims=True)
        delta = delta + row_grad * lax.rsqrt(state + mean_square + EPSILON)
        squares = squares + mean_square
        gains = gains + grad_ref[slots:].astype(f32)
    update_ref[...] = delta * (-LEARN_RATE / replicas)
    squares_row = jnp.sum(jnp.where(eye, squares, 0.0), axis=0, keepdims=True)
    gains_ref[...] = gains[:2] + gains[2:4]
    state_out_ref[...] = (state_row + squares_row / replicas).reshape(state_out_ref.shape)


def spread_kernel(step, replicas, part_ref, *refs):
    uvqk_ref, out_ref, uvqk_rows, out_rows, sems = refs[-5:]
    height, columns = uvqk_rows.shape
    width = out_rows.shape[1]
    part = lax.rem(lax.axis_index("replica") + (replicas - step), replicas)
    rows = pl.ds(pl.multiple_of(part * height, 8), height)
    blocks = columns // width
    for block in range(blocks):
        uvqk_rows[:, block * width : (block + 1) * width] = part_ref[
            block * height : (block + 1) * height
        ].astype(f32)
    first = pltpu.make_async_copy(uvqk_rows, uvqk_ref.at[rows], sems.at[0])
    first.start()
    out_rows[...] = part_ref[blocks * height : (blocks + 1) * height].astype(f32)
    second = pltpu.make_async_copy(out_rows, out_ref.at[rows], sems.at[1])
    second.start()
    first.wait()
    second.wait()


def hand_on(parts):
    replicas = len(parts)
    came = [parts[0]]
    for step in range(1, replicas):
        pairs = [(source, (source + step) % replicas) for source in range(replicas)]
        came.append(lax.ppermute(parts[step], "replica", pairs))
    return came


def from_all(value, replicas):
    came = hand_on([value] * replicas)
    if replicas > 2:
        order = lax.rem(lax.axis_index("replica") - jnp.arange(replicas) + replicas, replicas)
        stacked = jnp.take(jnp.stack(came), order, axis=0)
        came = [stacked[index] for index in range(replicas)]
    return came


def on_device(
    request_rows,
    token_slot,
    seq_lengths,
    cotangent,
    table_slab,
    adagrad_state,
    w_uvqk,
    w_out,
    norm_gain,
    out_gain,
):
    shards = lax.axis_size("shard")
    replicas = lax.axis_size("replica")
    tokens = token_slot.shape[1]
    rows_dev, width = table_slab.shape
    capacity = tokens // shards
    blocks = w_uvqk.shape[1] // width + 1
    share_rows = -(-blocks * width // (replicas * shards))
    part_rows = share_rows * shards
    grad_scale = 1.0 / math.sqrt(tokens * shards * replicas)
    shape = jax.ShapeDtypeStruct

    asked, small = pl.pallas_call(
        ready_kernel,
        out_shape=(
            shape((shards, 1, tokens), jnp.int32),
            shape((8, max(width, tokens)), f32),
        ),
        in_specs=[VMEM] * 5,
        out_specs=(VMEM, VMEM),
        cost_estimate=estimate(rows_dev * width * 8192, rows_dev * width * 128),
        compiler_params=room(4),
        name="ready",
    )(
        request_rows,
        token_slot,
        seq_lengths.reshape(1, -1),
        norm_gain.reshape(1, width),
        out_gain.reshape(1, width),
    )
    ids = lax.all_to_all(asked, "shard", split_axis=0, concat_axis=0, tiled=True)
    found, wanted = pl.pallas_call(
        functools.partial(fetch_kernel, capacity),
        out_shape=(shape((tokens, width), bf16), shape((1, tokens), f32)),
        in_specs=[VMEM] * 2,
        out_specs=(VMEM, VMEM),
        cost_estimate=estimate(2 * tokens * rows_dev * width, rows_dev * width * 4),
        compiler_params=room(8),
        name="fetch",
    )(ids, table_slab)
    slot_rows = lax.all_to_all(
        found.reshape(shards, capacity, width), "shard", split_axis=0, concat_axis=0, tiled=True
    ).reshape(tokens, width)

    cot = cotangent.reshape(tokens, width)
    lifted_grad, normal, gate_grad, *parts = pl.pallas_call(
        functools.partial(layer_kernel, seq_lengths.shape[-1]),
        out_shape=(
            shape((tokens, w_uvqk.shape[1]), bf16),
            shape((tokens, width + 128), f32),
            shape((1, width), f32),
        )
        + (shape((part_rows, width), bf16),) * replicas,
        in_specs=[VMEM] * 5,
        out_specs=(VMEM,) * (replicas + 3),
        scratch_shapes=[pltpu.VMEM((blocks * width, width), bf16)],
        cost_estimate=estimate(8 * tokens * width * w_uvqk.shape[1], 4 * blocks * width * width),
        compiler_params=room(20),
        name="layer",
    )(small, slot_rows, cot, w_uvqk, w_out)
    came = hand_on(parts)
    slot_grad, gain_rows = pl.pallas_call(
        finish_kernel,
        out_shape=(shape((tokens, width), bf16), shape((4, width), f32)),
        in_specs=[VMEM] * 6,
        out_specs=(VMEM, VMEM),
        cost_estimate=estimate(2 * tokens * width * w_uvqk.shape[1], 2 * blocks * width * width),
        compiler_params=room(10),
        name="finish",
    )(small, cot, w_uvqk, lifted_grad, normal, gate_grad)

    aligned = capacity % 8 == 0 and share_rows % 8 == 0
    message_rows = 2 * (capacity + share_rows) + GAIN_ROWS
    if aligned:
        message = pl.pallas_call(
            functools.partial(pack_kernel, shards),
            out_shape=shape((shards, message_rows, width // 2), bf16),
            in_specs=[VMEM] * (replicas + 2),
            out_specs=VMEM,
            compiler_params=room(10),
            name="pack",
        )(slot_grad, gain_rows, *came)
    else:
        total = sum(part.astype(f32) for part in came).astype(bf16)
        gains = jnp.broadcast_to(gain_rows.astype(bf16)[None], (shards, 4, width))
        message = jnp.concatenate(
            [
                slot_grad.reshape(shards, capacity, width),
                total.reshape(shards, share_rows, width),
                gains,
            ],
            axis=1,
        )
    arrived = lax.all_to_all(message, "shard", split_axis=0, concat_axis=0, tiled=True)
    if aligned:
        share = pl.pallas_call(
            functools.partial(unpack_kernel, capacity, grad_scale),
            out_shape=shape((shards, share_rows, width), bf16),
            in_specs=[VMEM],
            out_specs=VMEM,
            compiler_params=room(8),
            name="unpack",
        )(arrived)
        owned = pl.pallas_call(
            functools.partial(slots_kernel, capacity, grad_scale),
            out_shape=shape((tokens + GAIN_ROWS, width), bf16),
            in_specs=[VMEM],
            out_specs=VMEM,
            cost_estimate=estimate(tokens * width, 4 * tokens * width),
            compiler_params=room(6),
            name="slots",
        )(arrived)
    else:
        total = jnp.sum(arrived[:, capacity:].astype(f32), axis=0) * grad_scale
        share = jnp.broadcast_to(
            total[:share_rows].astype(bf16)[None], (shards, share_rows, width)
        )
        gains = total[share_rows : share_rows + 2] + total[share_rows + 2 :]
        high = gains.astype(bf16)
        owned = jnp.concatenate(
            [
                arrived[:, :capacity].reshape(tokens, width),
                high,
                (gains - high.astype(f32)).astype(bf16),
                jnp.zeros((GAIN_ROWS - 4, width), bf16),
            ],
            axis=0,
        )

    gathered = lax.all_to_all(share, "shard", split_axis=0, concat_axis=0, tiled=True)

    wanted_all = from_all(wanted, replicas)
    owned_all = from_all(owned, replicas)
    block = 128
    row_update, state_new, grad_gains = pl.pallas_call(
        functools.partial(adagrad_kernel, replicas),
        grid=(rows_dev // block,),
        out_shape=(
            shape((rows_dev, width), f32),
            shape((rows_dev // block, 1, block), f32),
            shape((2, width), f32),
        ),
        in_specs=[pl.BlockSpec((1, tokens), lambda step: (0, 0))] * replicas
        + [pl.BlockSpec((tokens + GAIN_ROWS, width), lambda step: (0, 0))] * replicas
        + [pl.BlockSpec((1, 1, block), lambda step: (step, 0, 0))],
        out_specs=(
            pl.BlockSpec((block, width), lambda step: (step, 0)),
            pl.BlockSpec((1, 1, block), lambda step: (step, 0, 0)),
            pl.BlockSpec((2, width), lambda step: (0, 0)),
        ),
        cost_estimate=estimate(2 * replicas * tokens * rows_dev * width, rows_dev * width * 4),
        compiler_params=room(10),
        name="adagrad",
    )(*wanted_all, *owned_all, adagrad_state.reshape(rows_dev // block, 1, block))

    halves = hand_on([gathered.reshape(part_rows, width)] * replicas)
    grads = ()
    for step, half in enumerate(halves):
        grads = pl.pallas_call(
            functools.partial(spread_kernel, step, replicas),
            out_shape=(shape(w_uvqk.shape, f32), shape(w_out.shape, f32)),
            in_specs=[VMEM] + [pl.BlockSpec(memory_space=pl.ANY)] * len(grads),
            out_specs=(pl.BlockSpec(memory_space=pl.ANY),) * 2,
            scratch_shapes=[
                pltpu.VMEM((width // replicas, w_uvqk.shape[1]), f32),
                pltpu.VMEM((width // replicas, width), f32),
                pltpu.SemaphoreType.DMA((2,)),
            ],
            input_output_aliases={1: 0, 2: 1} if grads else {},
            cost_estimate=estimate(blocks * width * width, 3 * blocks * width * width),
            compiler_params=room(6),
        )(half, *grads)
    return (row_update, state_new.reshape(rows_dev), *grads, grad_gains)


def solution(mesh):
    placed = (
        P("replica", "shard", None),
        P("replica", "shard"),
        P("replica", "shard", None),
        P("replica", "shard", None),
        P("shard", None),
        P("shard"),
        P(),
        P(),
        P(),
        P(),
    )

    return jax.shard_map(
        on_device,
        mesh=mesh,
        in_specs=placed,
        out_specs=(P("shard", None), P("shard"), P(), P(), P()),
        check_vma=False,
    )
```

```python
import functools
import math

import jax
import jax.numpy as jnp
from jax import lax
from jax.experimental import pallas as pl
from jax.experimental.pallas import tpu as pltpu
from jax.sharding import PartitionSpec as P


HEADS = 4
MAXLEN = 48
EPSILON = 1e-08
LEARN_RATE = 0.5
NORM_EPSILON = 1e-05
GAIN_ROWS = 8

f32 = jnp.float32
bf16 = jnp.bfloat16
VMEM = pl.BlockSpec(memory_space=pltpu.VMEM)


def room(mebibytes):
    return pltpu.CompilerParams(vmem_limit_bytes=mebibytes * 2**20)


def iota(shape, axis):
    return lax.broadcasted_iota(jnp.int32, shape, axis)


def mm(left, right, contract=(1, 0)):
    return lax.dot_general(
        left.astype(bf16),
        right.astype(bf16),
        (((contract[0],), (contract[1],)), ((), ())),
        preferred_element_type=f32,
    )


def estimate(flops, bytes_accessed):
    return pl.CostEstimate(flops=flops, bytes_accessed=bytes_accessed, transcendentals=0)


def ready_kernel(asked_ref, slot_ref, length_ref, norm_ref, gate_ref, ids_ref, small_ref):
    ids_ref[...] = jnp.broadcast_to(asked_ref[...], ids_ref.shape)
    small_ref[0:1, : slot_ref.shape[1]] = slot_ref[...].astype(f32)
    small_ref[1:2, : length_ref.shape[1]] = length_ref[...].astype(f32)
    small_ref[2:3, : norm_ref.shape[1]] = norm_ref[...]
    small_ref[3:4, : gate_ref.shape[1]] = gate_ref[...]


def fetch_kernel(capacity, ids_ref, table_ref, found_ref, wanted_ref):
    me = lax.axis_index("shard")
    ids = ids_ref[...].reshape(ids_ref.shape[0], ids_ref.shape[2])
    shards, slots = ids.shape
    rows = table_ref.shape[0]
    high = (ids >> 5).astype(f32)
    low = (ids & 31).astype(f32)
    slot = iota((slots, shards), 0)
    first = iota((slots, shards), 1) * capacity
    expand = ((slot >= first) & (slot < first + capacity)).astype(f32)
    asked = mm(expand, high) * 32.0 + mm(expand, low)
    pick = iota((slots, slots), 1) == me * capacity + lax.rem(iota((slots, slots), 0), capacity)
    column = jnp.sum(jnp.where(pick, asked, 0.0), axis=1, keepdims=True)
    eye = iota((slots, slots), 0) == iota((slots, slots), 1)
    wanted_ref[...] = jnp.sum(jnp.where(eye, column, 0.0), axis=0, keepdims=True)
    chosen = (column.astype(jnp.int32) == iota((slots, rows), 1)).astype(f32)
    found_ref[...] = mm(chosen, table_ref[...]).astype(bf16)


def center(values):
    shifted = values - jnp.mean(values, axis=1, keepdims=True)
    scale = lax.rsqrt(jnp.mean(shifted * shifted, axis=1, keepdims=True) + NORM_EPSILON)
    return shifted * scale, scale


def center_grad(grad, normal, scale):
    along = jnp.mean(grad * normal, axis=1, keepdims=True)
    return scale * (grad - jnp.mean(grad, axis=1, keepdims=True) - normal * along)


def sigmoid(values):
    return 1.0 / (1.0 + jnp.exp(-values))


def segments(lengths):
    count = lengths.shape[1]
    row, col = iota((count, count), 0), iota((count, count), 1)
    column = jnp.sum(jnp.where(row == col, lengths, 0.0), axis=1, keepdims=True)
    ends_column = jnp.sum(jnp.where(col <= row, lengths, 0.0), axis=1, keepdims=True)
    ends_row = jnp.sum(jnp.where(row <= col, column, 0.0), axis=0, keepdims=True)
    return ends_row, ends_column


def layer_kernel(
    histories, small_ref, rows_ref, cot_ref, w_ref, wo_ref, lifted_ref, normal_ref, gate_ref, *rest
):
    part_refs, stacked = rest[:-1], rest[-1]
    replicas = len(part_refs)
    tokens, width = rows_ref.shape
    head = width // HEADS
    row, col = iota((tokens, tokens), 0), iota((tokens, tokens), 1)

    slot_row = small_ref[0:1, :tokens]
    slot_column = jnp.sum(jnp.where(row == col, slot_row, 0.0), axis=1, keepdims=True)
    embedded = mm((slot_column.astype(jnp.int32) == col).astype(f32), rows_ref[...])

    ends_row, ends_column = segments(small_ref[1:2, :histories])
    before_row = iota((histories, tokens), 1).astype(f32) >= ends_column
    segment_row = jnp.sum(before_row.astype(f32), axis=0, keepdims=True)
    before_column = iota((tokens, histories), 0).astype(f32) >= ends_row
    segment_column = jnp.sum(before_column.astype(f32), axis=1, keepdims=True)
    same = (segment_row == segment_column) & (row >= col)
    same = jnp.concatenate([same.astype(f32)] * HEADS, axis=0)

    lane = iota((1, width), 1)
    heads = [((lane >= h * head) & (lane < (h + 1) * head)).astype(f32) for h in range(HEADS)]

    def by_head(values):
        return jnp.concatenate([values * mask for mask in heads], axis=0).astype(bf16)

    def beside(values):
        return jnp.concatenate(
            [values[h * tokens : (h + 1) * tokens] for h in range(HEADS)], axis=1
        )

    norm_gain, gate_gain = small_ref[2:3, :width], small_ref[3:4, :width]
    normal, scale = center(embedded)
    normed = (normal * norm_gain).astype(bf16)
    lifted = mm(normed, w_ref[...])
    sig = sigmoid(lifted)
    projected = lifted * sig
    slope = sig * (1.0 + lifted * (1.0 - sig))
    gate_u = projected[:, :width]
    values = projected[:, width : 2 * width].astype(bf16).astype(f32)
    queries = projected[:, 2 * width : 3 * width].astype(bf16).astype(f32)
    keys = projected[:, 3 * width :].astype(bf16).astype(f32)

    queries_by, keys_by, values_by = by_head(queries), by_head(keys), by_head(values)
    scores = mm(queries_by, keys, (1, 1)) * head ** (-0.5)
    score_sig = sigmoid(scores)
    weights = (same * (scores * score_sig / MAXLEN)).astype(bf16)
    attended = mm(beside(weights), values_by)
    normal_two, scale_two = center(attended)
    gated = (normal_two * gate_gain * gate_u).astype(bf16)

    cot = cot_ref[...]
    gated_grad = mm(cot, wo_ref[...], (1, 1)).astype(bf16).astype(f32)
    out_grad = mm(gated, cot, (0, 0))
    normal_u = normal_two * gate_u
    gate_ref[...] = jnp.sum(gated_grad * normal_u, axis=0, keepdims=True)
    gated_gain = gated_grad * gate_gain
    u_grad = gated_gain * normal_two
    attended_grad = center_grad(gated_gain * gate_u, normal_two, scale_two)
    attended_by = by_head(attended_grad)
    weights_grad = mm(attended_by, values, (1, 1)).astype(bf16).astype(f32)
    values_grad = mm(weights, attended_by, (0, 0)).astype(bf16).astype(f32)
    score_slope = score_sig * (1.0 + scores * (1.0 - score_sig))
    scores_grad = (same * weights_grad * score_slope * (head ** (-0.5) / MAXLEN)).astype(bf16)
    queries_grad = mm(beside(scores_grad), keys_by).astype(bf16).astype(f32)
    keys_grad = mm(scores_grad, queries_by, (0, 0)).astype(bf16).astype(f32)
    lifted_grad = (
        jnp.concatenate([u_grad, values_grad, queries_grad, keys_grad], axis=1) * slope
    ).astype(bf16)
    lifted_ref[...] = lifted_grad
    normal_ref[:, :width] = normal
    normal_ref[:, width:] = jnp.broadcast_to(scale, (tokens, normal_ref.shape[1] - width))
    w_grad = mm(normed, lifted_grad, (0, 0)).astype(bf16)

    blocks = w_grad.shape[1] // width
    for block in range(blocks):
        stacked[block * width : (block + 1) * width] = w_grad[:, block * width : (block + 1) * width]
    stacked[blocks * width :] = out_grad.astype(bf16)
    me = lax.axis_index("replica")
    height = width // replicas
    for step, part_ref in enumerate(part_refs):
        start = lax.rem(me + step, replicas) * height
        for block in range(blocks + 1):
            part_ref[block * height : (block + 1) * height] = stacked[
                pl.ds(pl.multiple_of(block * width + start, 16), height)
            ]
        filled = (blocks + 1) * height
        if filled < part_ref.shape[0]:
            part_ref[filled:] = jnp.zeros((part_ref.shape[0] - filled, width), bf16)


def finish_kernel(small_ref, cot_ref, w_ref, lifted_ref, normal_ref, gate_ref, slot_grad_ref, gain_ref):
    tokens, width = cot_ref.shape
    normal = normal_ref[:, :width]
    scale = normal_ref[:, width : width + 1]
    normed_grad = mm(lifted_ref[...], w_ref[...], (1, 1)).astype(bf16).astype(f32)
    norm_gain_grad = jnp.sum(normed_grad * normal, axis=0, keepdims=True)
    token_grad = cot_ref[...].astype(f32) + center_grad(
        normed_grad * small_ref[2:3, :width], normal, scale
    )
    slot_row = small_ref[0:1, :tokens].astype(jnp.int32)
    to_slot = (slot_row == iota((tokens, tokens), 0)).astype(f32)
    grad_high = token_grad.astype(bf16).astype(f32)
    slot_grad_ref[...] = mm(
        jnp.concatenate([to_slot, to_slot], axis=1),
        jnp.concatenate([grad_high, token_grad - grad_high], axis=0),
    ).astype(bf16)
    gains = jnp.concatenate([norm_gain_grad, gate_ref[...]], axis=0)
    high = gains.astype(bf16).astype(f32)
    gain_ref[...] = jnp.concatenate([high, gains - high], axis=0)


def halves_down(values):
    lanes = values.shape[-1] // 2
    return jnp.concatenate([values[..., :lanes], values[..., lanes:]], axis=-2)


def halves_across(values):
    rows = values.shape[-2] // 2
    return jnp.concatenate([values[..., :rows, :], values[..., rows:, :]], axis=-1)


def pack_kernel(group, slot_grad_ref, gain_ref, *refs):
    part_refs, out_ref = refs[:-1], refs[-1]
    half_slots, width = slot_grad_ref.shape[0] // 2, slot_grad_ref.shape[1]
    total = part_refs[0][...].astype(f32)
    for part_ref in part_refs[1:]:
        total = total + part_ref[...].astype(f32)
    half = lax.axis_index("shard") // group

    def slots_of(which):
        rows = pl.ds(pl.multiple_of(which * half_slots, 16), half_slots)
        return halves_down(slot_grad_ref[rows].astype(f32).reshape(group, -1, width))

    gains = halves_down(gain_ref[...])
    out_ref[...] = jnp.concatenate(
        [
            slots_of(half),
            slots_of(1 - half),
            halves_down(total.reshape(group, -1, width)),
            jnp.broadcast_to(gains[None], (group,) + gains.shape),
        ],
        axis=1,
    ).astype(bf16)


def as_two(values):
    high = values.astype(bf16).astype(f32)
    return jnp.concatenate([high, values - high], axis=0)


def cross_kernel(capacity, in_ref, cross_ref, mine_ref):
    group, _, lanes = in_ref.shape
    slots = 2 * capacity
    mine_ref[...] = halves_across(in_ref[:, :slots].astype(f32)).reshape(mine_ref.shape).astype(bf16)
    theirs = halves_across(in_ref[:, slots : 2 * slots].astype(f32)).reshape(mine_ref.shape)
    total = in_ref[0, 2 * slots :].astype(f32)
    for peer in range(1, group):
        total = total + in_ref[peer, 2 * slots :].astype(f32)
    gains = halves_across(total[-GAIN_ROWS:])
    gains = as_two(gains[:2] + gains[2:])
    padding = jnp.zeros((GAIN_ROWS - gains.shape[0], 2 * lanes), f32)
    share = halves_across(total[:-GAIN_ROWS])
    cross_ref[...] = jnp.concatenate([theirs, share, gains, padding], axis=0).astype(bf16)


def share_kernel(grad_scale, mine_ref, other_ref, share_ref):
    group, rows, _ = share_ref.shape
    first = mine_ref.shape[0] - GAIN_ROWS - rows
    total = mine_ref[first : first + rows].astype(f32) + other_ref[first : first + rows].astype(f32)
    share = (total * grad_scale).astype(bf16)
    for peer in range(group):
        share_ref[peer] = share


def slots_kernel(group, grad_scale, slots_ref, mine_ref, other_ref, owned_ref):
    rows = slots_ref.shape[0]
    half = lax.axis_index("shard") // group
    owned_ref[pl.ds(pl.multiple_of(half * rows, 16), rows)] = slots_ref[...]
    owned_ref[pl.ds(pl.multiple_of((1 - half) * rows, 16), rows)] = other_ref[:rows]
    gains = mine_ref[-GAIN_ROWS:].astype(f32) + other_ref[-GAIN_ROWS:].astype(f32)
    gains = as_two((gains[:2] + gains[2:4]) * grad_scale)
    padding = jnp.zeros((GAIN_ROWS - gains.shape[0], gains.shape[1]), f32)
    owned_ref[2 * rows :] = jnp.concatenate([gains, padding], axis=0).astype(bf16)


def adagrad_kernel(replicas, *refs):
    wanted_refs, grad_refs = refs[:replicas], refs[replicas : 2 * replicas]
    state_ref, update_ref, state_out_ref, gains_ref = refs[2 * replicas :]
    rows = update_ref.shape[0]
    slots = wanted_refs[0].shape[1]
    first = pl.program_id(0) * rows
    eye = iota((rows, rows), 0) == iota((rows, rows), 1)
    state_row = state_ref[...].reshape(1, rows)
    state = jnp.sum(jnp.where(eye, state_row, 0.0), axis=1, keepdims=True)
    delta = jnp.zeros(update_ref.shape, f32)
    squares = jnp.zeros((rows, 1), f32)
    gains = jnp.zeros((grad_refs[0].shape[0] - slots, update_ref.shape[1]), f32)
    for wanted_ref, grad_ref in zip(wanted_refs, grad_refs):
        hit = iota((rows, slots), 0) + first == wanted_ref[...].astype(jnp.int32)
        row_grad = mm(hit.astype(f32), grad_ref[:slots])
        mean_square = jnp.mean(row_grad * row_grad, axis=1, keepdims=True)
        delta = delta + row_grad * lax.rsqrt(state + mean_square + EPSILON)
        squares = squares + mean_square
        gains = gains + grad_ref[slots:].astype(f32)
    update_ref[...] = delta * (-LEARN_RATE / replicas)
    squares_row = jnp.sum(jnp.where(eye, squares, 0.0), axis=0, keepdims=True)
    gains_ref[...] = gains[:2] + gains[2:4]
    state_out_ref[...] = (state_row + squares_row / replicas).reshape(state_out_ref.shape)


def spread_kernel(step, replicas, part_ref, *refs):
    uvqk_ref, out_ref, uvqk_rows, out_rows, sems = refs[-5:]
    height, columns = uvqk_rows.shape
    width = out_rows.shape[1]
    part = lax.rem(lax.axis_index("replica") + (replicas - step), replicas)
    rows = pl.ds(pl.multiple_of(part * height, 8), height)
    blocks = columns // width
    for block in range(blocks):
        uvqk_rows[:, block * width : (block + 1) * width] = part_ref[
            block * height : (block + 1) * height
        ].astype(f32)
    first = pltpu.make_async_copy(uvqk_rows, uvqk_ref.at[rows], sems.at[0])
    first.start()
    out_rows[...] = part_ref[blocks * height : (blocks + 1) * height].astype(f32)
    second = pltpu.make_async_copy(out_rows, out_ref.at[rows], sems.at[1])
    second.start()
    first.wait()
    second.wait()


def hand_on(parts):
    replicas = len(parts)
    came = [parts[0]]
    for step in range(1, replicas):
        pairs = [(source, (source + step) % replicas) for source in range(replicas)]
        came.append(lax.ppermute(parts[step], "replica", pairs))
    return came


def from_all(value, replicas):
    came = hand_on([value] * replicas)
    if replicas > 2:
        order = lax.rem(lax.axis_index("replica") - jnp.arange(replicas) + replicas, replicas)
        stacked = jnp.take(jnp.stack(came), order, axis=0)
        came = [stacked[index] for index in range(replicas)]
    return came


def on_device(
    request_rows,
    token_slot,
    seq_lengths,
    cotangent,
    table_slab,
    adagrad_state,
    w_uvqk,
    w_out,
    norm_gain,
    out_gain,
):
    shards = lax.axis_size("shard")
    replicas = lax.axis_size("replica")
    tokens = token_slot.shape[1]
    rows_dev, width = table_slab.shape
    capacity = tokens // shards
    blocks = w_uvqk.shape[1] // width + 1
    group = shards // 2
    share_rows = -(-blocks * width // (replicas * group))
    part_rows = share_rows * group
    in_half = [list(range(group)), list(range(group, shards))]
    half_slots = group * capacity
    grad_scale = 1.0 / math.sqrt(tokens * shards * replicas)
    shape = jax.ShapeDtypeStruct

    asked, small = pl.pallas_call(
        ready_kernel,
        out_shape=(
            shape((shards, 1, tokens), jnp.int32),
            shape((8, max(width, tokens)), f32),
        ),
        in_specs=[VMEM] * 5,
        out_specs=(VMEM, VMEM),
        cost_estimate=estimate(rows_dev * width * 8192, rows_dev * width * 128),
        compiler_params=room(4),
        name="ready",
    )(
        request_rows,
        token_slot,
        seq_lengths.reshape(1, -1),
        norm_gain.reshape(1, width),
        out_gain.reshape(1, width),
    )
    ids = lax.all_to_all(asked, "shard", split_axis=0, concat_axis=0, tiled=True)
    found, wanted = pl.pallas_call(
        functools.partial(fetch_kernel, capacity),
        out_shape=(shape((tokens, width), bf16), shape((1, tokens), f32)),
        in_specs=[VMEM] * 2,
        out_specs=(VMEM, VMEM),
        cost_estimate=estimate(2 * tokens * rows_dev * width, rows_dev * width * 4),
        compiler_params=room(8),
        name="fetch",
    )(ids, table_slab)
    slot_rows = lax.all_to_all(
        found.reshape(shards, capacity, width), "shard", split_axis=0, concat_axis=0, tiled=True
    ).reshape(tokens, width)

    cot = cotangent.reshape(tokens, width)
    lifted_grad, normal, gate_grad, *parts = pl.pallas_call(
        functools.partial(layer_kernel, seq_lengths.shape[-1]),
        out_shape=(
            shape((tokens, w_uvqk.shape[1]), bf16),
            shape((tokens, width + 128), f32),
            shape((1, width), f32),
        )
        + (shape((part_rows, width), bf16),) * replicas,
        in_specs=[VMEM] * 5,
        out_specs=(VMEM,) * (replicas + 3),
        scratch_shapes=[pltpu.VMEM((blocks * width, width), bf16)],
        cost_estimate=estimate(8 * tokens * width * w_uvqk.shape[1], 4 * blocks * width * width),
        compiler_params=room(20),
        name="layer",
    )(small, slot_rows, cot, w_uvqk, w_out)
    came = hand_on(parts)
    slot_grad, gain_rows = pl.pallas_call(
        finish_kernel,
        out_shape=(shape((tokens, width), bf16), shape((4, width), f32)),
        in_specs=[VMEM] * 6,
        out_specs=(VMEM, VMEM),
        cost_estimate=estimate(2 * tokens * width * w_uvqk.shape[1], 2 * blocks * width * width),
        compiler_params=room(10),
        name="finish",
    )(small, cot, w_uvqk, lifted_grad, normal, gate_grad)

    aligned = capacity % 8 == 0 and share_rows % 8 == 0
    message_rows = 2 * (2 * capacity + share_rows) + GAIN_ROWS
    if aligned:
        message = pl.pallas_call(
            functools.partial(pack_kernel, group),
            out_shape=shape((group, message_rows, width // 2), bf16),
            in_specs=[VMEM] * (replicas + 2),
            out_specs=VMEM,
            compiler_params=room(10),
            name="pack",
        )(slot_grad, gain_rows, *came)
    else:
        half = lax.axis_index("shard") // group
        by_half = slot_grad.reshape(2, group, capacity, width)
        total = sum(part.astype(f32) for part in came).astype(bf16)
        message = jnp.concatenate(
            [
                jnp.take(by_half, half, axis=0),
                jnp.take(by_half, 1 - half, axis=0),
                total.reshape(group, share_rows, width),
                jnp.broadcast_to(gain_rows.astype(bf16)[None], (group, 4, width)),
            ],
            axis=1,
        )
    arrived = lax.all_to_all(
        message, "shard", split_axis=0, concat_axis=0, tiled=True, axis_index_groups=in_half
    )
    cross_rows = half_slots + share_rows + GAIN_ROWS
    if aligned:
        cross, mine = pl.pallas_call(
            functools.partial(cross_kernel, capacity),
            out_shape=(shape((cross_rows, width), bf16), shape((half_slots, width), bf16)),
            in_specs=[VMEM],
            out_specs=(VMEM, VMEM),
            compiler_params=room(8),
            name="cross",
        )(arrived)
    else:
        mine = arrived[:, :capacity].reshape(half_slots, width)
        theirs = arrived[:, capacity : 2 * capacity].reshape(half_slots, width)
        total = jnp.sum(arrived[:, 2 * capacity :].astype(f32), axis=0)
        gains = as_two(total[share_rows : share_rows + 2] + total[share_rows + 2 :]).astype(bf16)
        padding = jnp.zeros((GAIN_ROWS - 4, width), bf16)
        cross = jnp.concatenate([theirs, total[:share_rows].astype(bf16), gains, padding], axis=0)
    mirror = [(source, (source + group) % shards) for source in range(shards)]
    other = lax.ppermute(cross, "shard", mirror)
    if aligned:
        share = pl.pallas_call(
            functools.partial(share_kernel, grad_scale),
            out_shape=shape((group, share_rows, width), bf16),
            in_specs=[VMEM] * 2,
            out_specs=VMEM,
            compiler_params=room(4),
            name="share",
        )(cross, other)
        owned = pl.pallas_call(
            functools.partial(slots_kernel, group, grad_scale),
            out_shape=shape((tokens + GAIN_ROWS, width), bf16),
            in_specs=[VMEM] * 3,
            out_specs=VMEM,
            cost_estimate=estimate(tokens * width, 4 * tokens * width),
            compiler_params=room(4),
            name="slots",
        )(mine, cross, other)
    else:
        total = (cross[half_slots:].astype(f32) + other[half_slots:].astype(f32)) * grad_scale
        share = jnp.broadcast_to(
            total[:share_rows].astype(bf16)[None], (group, share_rows, width)
        )
        gains = as_two(total[share_rows : share_rows + 2] + total[share_rows + 2 : share_rows + 4])
        by_half = jnp.stack([mine, other[:half_slots]])
        by_half = jnp.where(half == 0, by_half, by_half[::-1]).reshape(tokens, width)
        owned = jnp.concatenate([by_half, gains.astype(bf16), padding], axis=0)

    gathered = lax.all_to_all(
        share, "shard", split_axis=0, concat_axis=0, tiled=True, axis_index_groups=in_half
    )

    wanted_all = from_all(wanted, replicas)
    owned_all = from_all(owned, replicas)
    block = 128
    row_update, state_new, grad_gains = pl.pallas_call(
        functools.partial(adagrad_kernel, replicas),
        grid=(rows_dev // block,),
        out_shape=(
            shape((rows_dev, width), f32),
            shape((rows_dev // block, 1, block), f32),
            shape((2, width), f32),
        ),
        in_specs=[pl.BlockSpec((1, tokens), lambda step: (0, 0))] * replicas
        + [pl.BlockSpec((tokens + GAIN_ROWS, width), lambda step: (0, 0))] * replicas
        + [pl.BlockSpec((1, 1, block), lambda step: (step, 0, 0))],
        out_specs=(
            pl.BlockSpec((block, width), lambda step: (step, 0)),
            pl.BlockSpec((1, 1, block), lambda step: (step, 0, 0)),
            pl.BlockSpec((2, width), lambda step: (0, 0)),
        ),
        cost_estimate=estimate(2 * replicas * tokens * rows_dev * width, rows_dev * width * 4),
        compiler_params=room(10),
        name="adagrad",
    )(*wanted_all, *owned_all, adagrad_state.reshape(rows_dev // block, 1, block))

    halves = hand_on([gathered.reshape(part_rows, width)] * replicas)
    grads = ()
    for step, half in enumerate(halves):
        grads = pl.pallas_call(
            functools.partial(spread_kernel, step, replicas),
            out_shape=(shape(w_uvqk.shape, f32), shape(w_out.shape, f32)),
            in_specs=[VMEM] + [pl.BlockSpec(memory_space=pl.ANY)] * len(grads),
            out_specs=(pl.BlockSpec(memory_space=pl.ANY),) * 2,
            scratch_shapes=[
                pltpu.VMEM((width // replicas, w_uvqk.shape[1]), f32),
                pltpu.VMEM((width // replicas, width), f32),
                pltpu.SemaphoreType.DMA((2,)),
            ],
            input_output_aliases={1: 0, 2: 1} if grads else {},
            cost_estimate=estimate(blocks * width * width, 3 * blocks * width * width),
            compiler_params=room(6),
        )(half, *grads)
    return (row_update, state_new.reshape(rows_dev), *grads, grad_gains)


def solution(mesh):
    placed = (
        P("replica", "shard", None),
        P("replica", "shard"),
        P("replica", "shard", None),
        P("replica", "shard", None),
        P("shard", None),
        P("shard"),
        P(),
        P(),
        P(),
        P(),
    )

    return jax.shard_map(
        on_device,
        mesh=mesh,
        in_specs=placed,
        out_specs=(P("shard", None), P("shard"), P(), P(), P()),
        check_vma=False,
    )
```

```python
import functools
import math

import jax
import jax.numpy as jnp
from jax import lax
from jax.experimental import pallas as pl
from jax.experimental.pallas import tpu as pltpu
from jax.sharding import PartitionSpec as P


HEADS = 4
MAXLEN = 48
EPSILON = 1e-08
LEARN_RATE = 0.5
NORM_EPSILON = 1e-05
GAIN_ROWS = 8

f32 = jnp.float32
bf16 = jnp.bfloat16
VMEM = pl.BlockSpec(memory_space=pltpu.VMEM)


def room(mebibytes):
    return pltpu.CompilerParams(vmem_limit_bytes=mebibytes * 2**20)


def iota(shape, axis):
    return lax.broadcasted_iota(jnp.int32, shape, axis)


def mm(left, right, contract=(1, 0)):
    return lax.dot_general(
        left.astype(bf16),
        right.astype(bf16),
        (((contract[0],), (contract[1],)), ((), ())),
        preferred_element_type=f32,
    )


def estimate(flops, bytes_accessed):
    return pl.CostEstimate(flops=flops, bytes_accessed=bytes_accessed, transcendentals=0)


def ready_kernel(asked_ref, slot_ref, length_ref, norm_ref, gate_ref, ids_ref, small_ref):
    ids_ref[...] = jnp.broadcast_to(asked_ref[...], ids_ref.shape)
    small_ref[0:1, : slot_ref.shape[1]] = slot_ref[...].astype(f32)
    small_ref[1:2, : length_ref.shape[1]] = length_ref[...].astype(f32)
    small_ref[2:3, : norm_ref.shape[1]] = norm_ref[...]
    small_ref[3:4, : gate_ref.shape[1]] = gate_ref[...]


def fetch_kernel(capacity, ids_ref, table_ref, found_ref, wanted_ref):
    me = lax.axis_index("shard")
    ids = ids_ref[...].reshape(ids_ref.shape[0], ids_ref.shape[2])
    shards, slots = ids.shape
    rows = table_ref.shape[0]
    high = (ids >> 5).astype(f32)
    low = (ids & 31).astype(f32)
    slot = iota((slots, shards), 0)
    first = iota((slots, shards), 1) * capacity
    expand = ((slot >= first) & (slot < first + capacity)).astype(f32)
    asked = mm(expand, high) * 32.0 + mm(expand, low)
    pick = iota((slots, slots), 1) == me * capacity + lax.rem(iota((slots, slots), 0), capacity)
    column = jnp.sum(jnp.where(pick, asked, 0.0), axis=1, keepdims=True)
    eye = iota((slots, slots), 0) == iota((slots, slots), 1)
    wanted_ref[...] = jnp.sum(jnp.where(eye, column, 0.0), axis=0, keepdims=True)
    chosen = (column.astype(jnp.int32) == iota((slots, rows), 1)).astype(f32)
    found_ref[...] = mm(chosen, table_ref[...]).astype(bf16)


def center(values):
    shifted = values - jnp.mean(values, axis=1, keepdims=True)
    scale = lax.rsqrt(jnp.mean(shifted * shifted, axis=1, keepdims=True) + NORM_EPSILON)
    return shifted * scale, scale


def center_grad(grad, normal, scale):
    along = jnp.mean(grad * normal, axis=1, keepdims=True)
    return scale * (grad - jnp.mean(grad, axis=1, keepdims=True) - normal * along)


def sigmoid(values):
    return 0.5 + 0.5 * jnp.tanh(0.5 * values)


def segments(lengths):
    count = lengths.shape[1]
    row, col = iota((count, count), 0), iota((count, count), 1)
    column = jnp.sum(jnp.where(row == col, lengths, 0.0), axis=1, keepdims=True)
    ends_column = jnp.sum(jnp.where(col <= row, lengths, 0.0), axis=1, keepdims=True)
    ends_row = jnp.sum(jnp.where(row <= col, column, 0.0), axis=0, keepdims=True)
    return ends_row, ends_column


def part_of_grads(part, height, left_ref, lifted_grad, cot, part_ref):
    width = cot.shape[1]
    blocks = lifted_grad.shape[1] // width
    features = left_ref.shape[0] // 2
    start = pl.multiple_of(part * height, 16)
    w_grad = mm(left_ref[pl.ds(start, height)], lifted_grad).astype(bf16)
    for block in range(blocks):
        part_ref[block * height : (block + 1) * height] = w_grad[:, block * width : (block + 1) * width]
    out_grad = mm(left_ref[pl.ds(pl.multiple_of(features + start, 16), height)], cot).astype(bf16)
    part_ref[blocks * height : (blocks + 1) * height] = out_grad
    filled = (blocks + 1) * height
    if filled < part_ref.shape[0]:
        part_ref[filled:] = jnp.zeros((part_ref.shape[0] - filled, width), bf16)


def layer_kernel(
    histories,
    small_ref,
    rows_ref,
    cot_ref,
    w_ref,
    wo_ref,
    lifted_ref,
    normal_ref,
    gate_ref,
    left_ref,
    *part_refs,
):
    replicas = len(part_refs) + 1
    tokens, width = rows_ref.shape
    head = width // HEADS
    row, col = iota((tokens, tokens), 0), iota((tokens, tokens), 1)

    slot_row = small_ref[0:1, :tokens]
    slot_column = jnp.sum(jnp.where(row == col, slot_row, 0.0), axis=1, keepdims=True)
    embedded = mm((slot_column.astype(jnp.int32) == col).astype(f32), rows_ref[...])

    ends_row, ends_column = segments(small_ref[1:2, :histories])
    before_row = iota((histories, tokens), 1).astype(f32) >= ends_column
    segment_row = jnp.sum(before_row.astype(f32), axis=0, keepdims=True)
    before_column = iota((tokens, histories), 0).astype(f32) >= ends_row
    segment_column = jnp.sum(before_column.astype(f32), axis=1, keepdims=True)
    same = (segment_row == segment_column) & (row >= col)
    same = jnp.concatenate([same.astype(f32)] * HEADS, axis=0)

    lane = iota((1, width), 1)
    heads = [((lane >= h * head) & (lane < (h + 1) * head)).astype(f32) for h in range(HEADS)]

    def by_head(values):
        return jnp.concatenate([values * mask for mask in heads], axis=0).astype(bf16)

    def beside(values):
        return jnp.concatenate(
            [values[h * tokens : (h + 1) * tokens] for h in range(HEADS)], axis=1
        )

    norm_gain, gate_gain = small_ref[2:3, :width], small_ref[3:4, :width]
    normal, scale = center(embedded)
    scaled = normal * norm_gain
    normed = scaled.astype(bf16)
    left_ref[:width] = scaled.T.astype(bf16)
    lifted = mm(normed, w_ref[...])
    sig = sigmoid(lifted)
    projected = lifted * sig
    slope = sig * (1.0 + lifted * (1.0 - sig))
    gate_u = projected[:, :width]
    values = projected[:, width : 2 * width].astype(bf16).astype(f32)
    queries = projected[:, 2 * width : 3 * width].astype(bf16).astype(f32)
    keys = projected[:, 3 * width :].astype(bf16).astype(f32)

    queries_by, keys_by, values_by = by_head(queries), by_head(keys), by_head(values)
    scores = mm(queries_by, keys, (1, 1)) * head ** (-0.5)
    score_sig = sigmoid(scores)
    weights = (same * (scores * score_sig / MAXLEN)).astype(bf16)
    attended = mm(beside(weights), values_by)
    normal_two, scale_two = center(attended)
    left_ref[width:] = (normal_two * gate_gain * gate_u).T.astype(bf16)

    cot = cot_ref[...]
    gated_grad = mm(cot, wo_ref[...], (1, 1)).astype(bf16).astype(f32)
    normal_u = normal_two * gate_u
    gate_ref[...] = jnp.sum(gated_grad * normal_u, axis=0, keepdims=True)
    gated_gain = gated_grad * gate_gain
    u_grad = gated_gain * normal_two
    attended_grad = center_grad(gated_gain * gate_u, normal_two, scale_two)
    attended_by = by_head(attended_grad)
    weights_grad = mm(attended_by, values, (1, 1)).astype(bf16).astype(f32)
    values_grad = mm(weights, attended_by, (0, 0)).astype(bf16).astype(f32)
    score_slope = score_sig * (1.0 + scores * (1.0 - score_sig))
    scores_grad = (same * weights_grad * score_slope * (head ** (-0.5) / MAXLEN)).astype(bf16)
    queries_grad = mm(beside(scores_grad), keys_by).astype(bf16).astype(f32)
    keys_grad = mm(scores_grad, queries_by, (0, 0)).astype(bf16).astype(f32)
    lifted_grad = (
        jnp.concatenate([u_grad, values_grad, queries_grad, keys_grad], axis=1) * slope
    ).astype(bf16)
    lifted_ref[...] = lifted_grad
    normal_ref[:, :width] = normal
    normal_ref[:, width:] = jnp.broadcast_to(scale, (tokens, normal_ref.shape[1] - width))
    me = lax.axis_index("replica")
    for step, part_ref in enumerate(part_refs, 1):
        part = lax.rem(me + step, replicas)
        part_of_grads(part, width // replicas, left_ref, lifted_grad, cot, part_ref)


def finish_kernel(
    replicas,
    small_ref,
    cot_ref,
    w_ref,
    lifted_ref,
    normal_ref,
    gate_ref,
    left_ref,
    slot_grad_ref,
    gain_ref,
    part_ref,
):
    tokens, width = cot_ref.shape
    me = lax.axis_index("replica")
    part_of_grads(me, width // replicas, left_ref, lifted_ref[...], cot_ref[...], part_ref)
    normal = normal_ref[:, :width]
    scale = normal_ref[:, width : width + 1]
    normed_grad = mm(lifted_ref[...], w_ref[...], (1, 1)).astype(bf16).astype(f32)
    norm_gain_grad = jnp.sum(normed_grad * normal, axis=0, keepdims=True)
    token_grad = cot_ref[...].astype(f32) + center_grad(
        normed_grad * small_ref[2:3, :width], normal, scale
    )
    slot_row = small_ref[0:1, :tokens].astype(jnp.int32)
    to_slot = (slot_row == iota((tokens, tokens), 0)).astype(f32)
    grad_high = token_grad.astype(bf16).astype(f32)
    slot_grad_ref[...] = mm(
        jnp.concatenate([to_slot, to_slot], axis=1),
        jnp.concatenate([grad_high, token_grad - grad_high], axis=0),
    ).astype(bf16)
    gains = jnp.concatenate([norm_gain_grad, gate_ref[...]], axis=0)
    high = gains.astype(bf16).astype(f32)
    gain_ref[...] = jnp.concatenate([high, gains - high], axis=0)


def halves_down(values):
    lanes = values.shape[-1] // 2
    return jnp.concatenate([values[..., :lanes], values[..., lanes:]], axis=-2)


def halves_across(values):
    rows = values.shape[-2] // 2
    return jnp.concatenate([values[..., :rows, :], values[..., rows:, :]], axis=-1)


def pack_kernel(group, slot_grad_ref, gain_ref, *refs):
    part_refs, out_ref = refs[:-1], refs[-1]
    half_slots, width = slot_grad_ref.shape[0] // 2, slot_grad_ref.shape[1]
    total = part_refs[0][...].astype(f32)
    for part_ref in part_refs[1:]:
        total = total + part_ref[...].astype(f32)
    half = lax.axis_index("shard") // group

    def slots_of(which):
        rows = pl.ds(pl.multiple_of(which * half_slots, 16), half_slots)
        return halves_down(slot_grad_ref[rows].astype(f32).reshape(group, -1, width))

    gains = halves_down(gain_ref[...])
    out_ref[...] = jnp.concatenate(
        [
            slots_of(half),
            slots_of(1 - half),
            halves_down(total.reshape(group, -1, width)),
            jnp.broadcast_to(gains[None], (group,) + gains.shape),
        ],
        axis=1,
    ).astype(bf16)


def as_two(values):
    high = values.astype(bf16).astype(f32)
    return jnp.concatenate([high, values - high], axis=0)


def cross_kernel(capacity, in_ref, cross_ref, theirs_ref, mine_ref):
    group, _, lanes = in_ref.shape
    slots = 2 * capacity
    mine_ref[...] = halves_across(in_ref[:, :slots].astype(f32)).reshape(mine_ref.shape).astype(bf16)
    theirs = halves_across(in_ref[:, slots : 2 * slots].astype(f32)).reshape(mine_ref.shape)
    total = in_ref[0, 2 * slots :].astype(f32)
    for peer in range(1, group):
        total = total + in_ref[peer, 2 * slots :].astype(f32)
    gains = halves_across(total[-GAIN_ROWS:])
    gains = as_two(gains[:2] + gains[2:])
    padding = jnp.zeros((GAIN_ROWS - gains.shape[0], 2 * lanes), f32)
    cross_ref[...] = halves_across(total[:-GAIN_ROWS]).astype(bf16)
    theirs_ref[...] = jnp.concatenate([theirs, gains, padding], axis=0).astype(bf16)


def share_kernel(grad_scale, mine_ref, other_ref, share_ref):
    group, _, _ = share_ref.shape
    total = mine_ref[...].astype(f32) + other_ref[...].astype(f32)
    share = (total * grad_scale).astype(bf16)
    for peer in range(group):
        share_ref[peer] = share


def slots_kernel(group, grad_scale, slots_ref, theirs_ref, other_ref, owned_ref):
    rows = slots_ref.shape[0]
    half = lax.axis_index("shard") // group
    owned_ref[pl.ds(pl.multiple_of(half * rows, 16), rows)] = slots_ref[...]
    owned_ref[pl.ds(pl.multiple_of((1 - half) * rows, 16), rows)] = other_ref[:rows]
    gains = theirs_ref[-GAIN_ROWS:].astype(f32) + other_ref[-GAIN_ROWS:].astype(f32)
    gains = as_two((gains[:2] + gains[2:4]) * grad_scale)
    padding = jnp.zeros((GAIN_ROWS - gains.shape[0], gains.shape[1]), f32)
    owned_ref[2 * rows :] = jnp.concatenate([gains, padding], axis=0).astype(bf16)


def adagrad_kernel(replicas, *refs):
    wanted_refs, grad_refs = refs[:replicas], refs[replicas : 2 * replicas]
    state_ref, update_ref, state_out_ref, gains_ref = refs[2 * replicas :]
    rows = update_ref.shape[0]
    chunks, _, lanes = state_ref.shape
    slots = wanted_refs[0].shape[1]
    first = pl.program_id(0) * rows
    eye = iota((lanes, lanes), 0) == iota((lanes, lanes), 1)
    state = jnp.concatenate(
        [
            jnp.sum(jnp.where(eye, state_ref[chunk], 0.0), axis=1, keepdims=True)
            for chunk in range(chunks)
        ],
        axis=0,
    )
    delta = jnp.zeros(update_ref.shape, f32)
    squares = jnp.zeros((rows, 1), f32)
    gains = jnp.zeros((grad_refs[0].shape[0] - slots, update_ref.shape[1]), f32)
    for wanted_ref, grad_ref in zip(wanted_refs, grad_refs):
        hit = iota((rows, slots), 0) + first == wanted_ref[...].astype(jnp.int32)
        row_grad = mm(hit.astype(f32), grad_ref[:slots])
        mean_square = jnp.mean(row_grad * row_grad, axis=1, keepdims=True)
        delta = delta + row_grad * lax.rsqrt(state + mean_square + EPSILON)
        squares = squares + mean_square
        gains = gains + grad_ref[slots:].astype(f32)
    update_ref[...] = delta * (-LEARN_RATE / replicas)
    for chunk in range(chunks):
        column = squares[chunk * lanes : (chunk + 1) * lanes]
        square_row = jnp.sum(jnp.where(eye, column, 0.0), axis=0, keepdims=True)
        state_out_ref[chunk] = state_ref[chunk] + square_row / replicas
    gains_ref[...] = gains[:2] + gains[2:4]


def spread_kernel(step, replicas, part_ref, *refs):
    uvqk_ref, out_ref, uvqk_rows, out_rows, sems = refs[-5:]
    height, columns = uvqk_rows.shape
    width = out_rows.shape[1]
    part = lax.rem(lax.axis_index("replica") + (replicas - step), replicas)
    rows = pl.ds(pl.multiple_of(part * height, 8), height)
    blocks = columns // width
    for block in range(blocks):
        uvqk_rows[:, block * width : (block + 1) * width] = part_ref[
            block * height : (block + 1) * height
        ].astype(f32)
    first = pltpu.make_async_copy(uvqk_rows, uvqk_ref.at[rows], sems.at[0])
    first.start()
    out_rows[...] = part_ref[blocks * height : (blocks + 1) * height].astype(f32)
    second = pltpu.make_async_copy(out_rows, out_ref.at[rows], sems.at[1])
    second.start()
    first.wait()
    second.wait()


def hand_on(parts):
    replicas = len(parts)
    came = [parts[0]]
    for step in range(1, replicas):
        pairs = [(source, (source + step) % replicas) for source in range(replicas)]
        came.append(lax.ppermute(parts[step], "replica", pairs))
    return came


def from_all(value, replicas):
    came = hand_on([value] * replicas)
    if replicas > 2:
        order = lax.rem(lax.axis_index("replica") - jnp.arange(replicas) + replicas, replicas)
        stacked = jnp.take(jnp.stack(came), order, axis=0)
        came = [stacked[index] for index in range(replicas)]
    return came


def on_device(
    request_rows,
    token_slot,
    seq_lengths,
    cotangent,
    table_slab,
    adagrad_state,
    w_uvqk,
    w_out,
    norm_gain,
    out_gain,
):
    shards = lax.axis_size("shard")
    replicas = lax.axis_size("replica")
    tokens = token_slot.shape[1]
    rows_dev, width = table_slab.shape
    capacity = tokens // shards
    blocks = w_uvqk.shape[1] // width + 1
    group = shards // 2
    share_rows = -(-blocks * width // (replicas * group))
    part_rows = share_rows * group
    in_half = [list(range(group)), list(range(group, shards))]
    half_slots = group * capacity
    grad_scale = 1.0 / math.sqrt(tokens * shards * replicas)
    shape = jax.ShapeDtypeStruct

    asked, small = pl.pallas_call(
        ready_kernel,
        out_shape=(
            shape((shards, 1, tokens), jnp.int32),
            shape((8, max(width, tokens)), f32),
        ),
        in_specs=[VMEM] * 5,
        out_specs=(VMEM, VMEM),
        cost_estimate=estimate(rows_dev * width * 8192, rows_dev * width * 128),
        compiler_params=room(4),
        name="ready",
    )(
        request_rows,
        token_slot,
        seq_lengths.reshape(1, -1),
        norm_gain.reshape(1, width),
        out_gain.reshape(1, width),
    )
    ids = lax.all_to_all(asked, "shard", split_axis=0, concat_axis=0, tiled=True)
    found, wanted = pl.pallas_call(
        functools.partial(fetch_kernel, capacity),
        out_shape=(shape((tokens, width), bf16), shape((1, tokens), f32)),
        in_specs=[VMEM] * 2,
        out_specs=(VMEM, VMEM),
        cost_estimate=estimate(2 * tokens * rows_dev * width, rows_dev * width * 4),
        compiler_params=room(8),
        name="fetch",
    )(ids, table_slab)
    slot_rows = lax.all_to_all(
        found.reshape(shards, capacity, width), "shard", split_axis=0, concat_axis=0, tiled=True
    ).reshape(tokens, width)

    cot = cotangent.reshape(tokens, width)
    lifted_grad, normal, gate_grad, left, *parts = pl.pallas_call(
        functools.partial(layer_kernel, seq_lengths.shape[-1]),
        out_shape=(
            shape((tokens, w_uvqk.shape[1]), bf16),
            shape((tokens, width + 128), f32),
            shape((1, width), f32),
            shape((2 * width, tokens), bf16),
        )
        + (shape((part_rows, width), bf16),) * (replicas - 1),
        in_specs=[VMEM] * 5,
        out_specs=(VMEM,) * (replicas + 3),
        cost_estimate=estimate(8 * tokens * width * w_uvqk.shape[1], 4 * blocks * width * width),
        compiler_params=room(20),
        name="layer",
    )(small, slot_rows, cot, w_uvqk, w_out)
    came = hand_on([None] + parts)[1:]
    slot_grad, gain_rows, kept = pl.pallas_call(
        functools.partial(finish_kernel, replicas),
        out_shape=(
            shape((tokens, width), bf16),
            shape((4, width), f32),
            shape((part_rows, width), bf16),
        ),
        in_specs=[VMEM] * 7,
        out_specs=(VMEM,) * 3,
        cost_estimate=estimate(3 * tokens * width * w_uvqk.shape[1], 3 * blocks * width * width),
        compiler_params=room(10),
        name="finish",
    )(small, cot, w_uvqk, lifted_grad, normal, gate_grad, left)
    came = [kept] + came

    aligned = capacity % 8 == 0 and share_rows % 8 == 0
    message_rows = 2 * (2 * capacity + share_rows) + GAIN_ROWS
    if aligned:
        message = pl.pallas_call(
            functools.partial(pack_kernel, group),
            out_shape=shape((group, message_rows, width // 2), bf16),
            in_specs=[VMEM] * (replicas + 2),
            out_specs=VMEM,
            compiler_params=room(10),
            name="pack",
        )(slot_grad, gain_rows, *came)
    else:
        half = lax.axis_index("shard") // group
        by_half = slot_grad.reshape(2, group, capacity, width)
        total = sum(part.astype(f32) for part in came).astype(bf16)
        message = jnp.concatenate(
            [
                jnp.take(by_half, half, axis=0),
                jnp.take(by_half, 1 - half, axis=0),
                total.reshape(group, share_rows, width),
                jnp.broadcast_to(gain_rows.astype(bf16)[None], (group, 4, width)),
            ],
            axis=1,
        )
    arrived = lax.all_to_all(
        message, "shard", split_axis=0, concat_axis=0, tiled=True, axis_index_groups=in_half
    )
    if aligned:
        cross, theirs, mine = pl.pallas_call(
            functools.partial(cross_kernel, capacity),
            out_shape=(
                shape((share_rows, width), bf16),
                shape((half_slots + GAIN_ROWS, width), bf16),
                shape((half_slots, width), bf16),
            ),
            in_specs=[VMEM],
            out_specs=(VMEM,) * 3,
            compiler_params=room(8),
            name="cross",
        )(arrived)
    else:
        mine = arrived[:, :capacity].reshape(half_slots, width)
        theirs = arrived[:, capacity : 2 * capacity].reshape(half_slots, width)
        total = jnp.sum(arrived[:, 2 * capacity :].astype(f32), axis=0)
        gains = as_two(total[share_rows : share_rows + 2] + total[share_rows + 2 :]).astype(bf16)
        padding = jnp.zeros((GAIN_ROWS - 4, width), bf16)
        cross = total[:share_rows].astype(bf16)
        theirs = jnp.concatenate([theirs, gains, padding], axis=0)
    mirror = [(source, (source + group) % shards) for source in range(shards)]
    other = lax.ppermute(cross, "shard", mirror)
    other_slots = lax.ppermute(theirs, "shard", mirror)
    if aligned:
        share = pl.pallas_call(
            functools.partial(share_kernel, grad_scale),
            out_shape=shape((group, share_rows, width), bf16),
            in_specs=[VMEM] * 2,
            out_specs=VMEM,
            compiler_params=room(4),
            name="share",
        )(cross, other)
        owned = pl.pallas_call(
            functools.partial(slots_kernel, group, grad_scale),
            out_shape=shape((tokens + GAIN_ROWS, width), bf16),
            in_specs=[VMEM] * 3,
            out_specs=VMEM,
            cost_estimate=estimate(tokens * width, 4 * tokens * width),
            compiler_params=room(4),
            name="slots",
        )(mine, theirs, other_slots)
    else:
        total = (cross.astype(f32) + other.astype(f32)) * grad_scale
        share = jnp.broadcast_to(total.astype(bf16)[None], (group, share_rows, width))
        gains = theirs[half_slots:].astype(f32) + other_slots[half_slots:].astype(f32)
        gains = as_two((gains[:2] + gains[2:4]) * grad_scale)
        by_half = jnp.stack([mine, other_slots[:half_slots]])
        by_half = jnp.where(half == 0, by_half, by_half[::-1]).reshape(tokens, width)
        owned = jnp.concatenate([by_half, gains.astype(bf16), padding], axis=0)

    gathered = lax.all_to_all(
        share, "shard", split_axis=0, concat_axis=0, tiled=True, axis_index_groups=in_half
    )

    wanted_all = from_all(wanted, replicas)
    owned_all = from_all(owned, replicas)
    lanes = 128
    block = min(rows_dev, 2048 // replicas)
    row_update, state_new, grad_gains = pl.pallas_call(
        functools.partial(adagrad_kernel, replicas),
        grid=(rows_dev // block,),
        out_shape=(
            shape((rows_dev, width), f32),
            shape((rows_dev // lanes, 1, lanes), f32),
            shape((2, width), f32),
        ),
        in_specs=[pl.BlockSpec((1, tokens), lambda step: (0, 0))] * replicas
        + [pl.BlockSpec((tokens + GAIN_ROWS, width), lambda step: (0, 0))] * replicas
        + [pl.BlockSpec((block // lanes, 1, lanes), lambda step: (step, 0, 0))],
        out_specs=(
            pl.BlockSpec((block, width), lambda step: (step, 0)),
            pl.BlockSpec((block // lanes, 1, lanes), lambda step: (step, 0, 0)),
            pl.BlockSpec((2, width), lambda step: (0, 0)),
        ),
        cost_estimate=estimate(2 * replicas * tokens * rows_dev * width, rows_dev * width * 4),
        compiler_params=room(12),
        name="adagrad",
    )(*wanted_all, *owned_all, adagrad_state.reshape(rows_dev // lanes, 1, lanes))

    halves = hand_on([gathered.reshape(part_rows, width)] * replicas)
    grads = ()
    for step, half in enumerate(halves):
        grads = pl.pallas_call(
            functools.partial(spread_kernel, step, replicas),
            out_shape=(shape(w_uvqk.shape, f32), shape(w_out.shape, f32)),
            in_specs=[VMEM] + [pl.BlockSpec(memory_space=pl.ANY)] * len(grads),
            out_specs=(pl.BlockSpec(memory_space=pl.ANY),) * 2,
            scratch_shapes=[
                pltpu.VMEM((width // replicas, w_uvqk.shape[1]), f32),
                pltpu.VMEM((width // replicas, width), f32),
                pltpu.SemaphoreType.DMA((2,)),
            ],
            input_output_aliases={1: 0, 2: 1} if grads else {},
            cost_estimate=estimate(blocks * width * width, 3 * blocks * width * width),
            compiler_params=room(6),
        )(half, *grads)
    return (row_update, state_new.reshape(rows_dev), *grads, grad_gains)


def solution(mesh):
    placed = (
        P("replica", "shard", None),
        P("replica", "shard"),
        P("replica", "shard", None),
        P("replica", "shard", None),
        P("shard", None),
        P("shard"),
        P(),
        P(),
        P(),
        P(),
    )

    return jax.shard_map(
        on_device,
        mesh=mesh,
        in_specs=placed,
        out_specs=(P("shard", None), P("shard"), P(), P(), P()),
        check_vma=False,
    )
```

```python
import functools
import math

import jax
import jax.numpy as jnp
from jax import lax
from jax.experimental import pallas as pl
from jax.experimental.pallas import tpu as pltpu
from jax.sharding import PartitionSpec as P


HEADS = 4
MAXLEN = 48
EPSILON = 1e-08
LEARN_RATE = 0.5
NORM_EPSILON = 1e-05
GAIN_ROWS = 8

f32 = jnp.float32
bf16 = jnp.bfloat16
VMEM = pl.BlockSpec(memory_space=pltpu.VMEM)


def room(mebibytes):
    return pltpu.CompilerParams(vmem_limit_bytes=mebibytes * 2**20)


def iota(shape, axis):
    return lax.broadcasted_iota(jnp.int32, shape, axis)


def mm(left, right, contract=(1, 0)):
    return lax.dot_general(
        left.astype(bf16),
        right.astype(bf16),
        (((contract[0],), (contract[1],)), ((), ())),
        preferred_element_type=f32,
    )


def estimate(flops, bytes_accessed):
    return pl.CostEstimate(flops=flops, bytes_accessed=bytes_accessed, transcendentals=0)


def ready_kernel(asked_ref, slot_ref, length_ref, norm_ref, gate_ref, ids_ref, small_ref):
    ids_ref[...] = jnp.broadcast_to(asked_ref[...], ids_ref.shape)
    small_ref[0:1, : slot_ref.shape[1]] = slot_ref[...].astype(f32)
    small_ref[1:2, : length_ref.shape[1]] = length_ref[...].astype(f32)
    small_ref[2:3, : norm_ref.shape[1]] = norm_ref[...]
    small_ref[3:4, : gate_ref.shape[1]] = gate_ref[...]


def segments(lengths):
    count = lengths.shape[1]
    row, col = iota((count, count), 0), iota((count, count), 1)
    column = jnp.sum(jnp.where(row == col, lengths, 0.0), axis=1, keepdims=True)
    ends_column = jnp.sum(jnp.where(col <= row, lengths, 0.0), axis=1, keepdims=True)
    ends_row = jnp.sum(jnp.where(row <= col, column, 0.0), axis=0, keepdims=True)
    return ends_row, ends_column


def token_kernel(histories, small_ref, token_ref, same_ref):
    tokens = token_ref.shape[0]
    row, col = iota((tokens, tokens), 0), iota((tokens, tokens), 1)
    slot_row = small_ref[0:1, :tokens]
    slot_column = jnp.sum(jnp.where(row == col, slot_row, 0.0), axis=1, keepdims=True)
    token_ref[...] = (slot_column.astype(jnp.int32) == col).astype(f32).astype(bf16)
    ends_row, ends_column = segments(small_ref[1:2, :histories])
    before_row = iota((histories, tokens), 1).astype(f32) >= ends_column
    segment_row = jnp.sum(before_row.astype(f32), axis=0, keepdims=True)
    before_column = iota((tokens, histories), 0).astype(f32) >= ends_row
    segment_column = jnp.sum(before_column.astype(f32), axis=1, keepdims=True)
    same_ref[...] = ((segment_row == segment_column) & (row >= col)).astype(f32)


def fetch_kernel(
    capacity, histories, ids_ref, table_ref, small_ref, found_ref, wanted_ref, token_ref, same_ref
):
    token_kernel(histories, small_ref, token_ref, same_ref)
    me = lax.axis_index("shard")
    ids = ids_ref[...].reshape(ids_ref.shape[0], ids_ref.shape[2])
    shards, slots = ids.shape
    rows = table_ref.shape[0]
    high = (ids >> 5).astype(f32)
    low = (ids & 31).astype(f32)
    slot = iota((slots, shards), 0)
    first = iota((slots, shards), 1) * capacity
    expand = ((slot >= first) & (slot < first + capacity)).astype(f32)
    asked = mm(expand, high) * 32.0 + mm(expand, low)
    pick = iota((slots, slots), 1) == me * capacity + lax.rem(iota((slots, slots), 0), capacity)
    column = jnp.sum(jnp.where(pick, asked, 0.0), axis=1, keepdims=True)
    eye = iota((slots, slots), 0) == iota((slots, slots), 1)
    wanted_ref[...] = jnp.sum(jnp.where(eye, column, 0.0), axis=0, keepdims=True)
    chosen = (column.astype(jnp.int32) == iota((slots, rows), 1)).astype(f32)
    found_ref[...] = mm(chosen, table_ref[...]).astype(bf16)


def center(values):
    shifted = values - jnp.mean(values, axis=1, keepdims=True)
    scale = lax.rsqrt(jnp.mean(shifted * shifted, axis=1, keepdims=True) + NORM_EPSILON)
    return shifted * scale, scale


def center_grad(grad, normal, scale):
    along = jnp.mean(grad * normal, axis=1, keepdims=True)
    return scale * (grad - jnp.mean(grad, axis=1, keepdims=True) - normal * along)


def sigmoid(values):
    return 0.5 + 0.5 * jnp.tanh(0.5 * values)


def part_of_grads(part, height, left_ref, lifted_grad, cot, part_ref):
    width = cot.shape[1]
    blocks = lifted_grad.shape[1] // width
    features = left_ref.shape[0] // 2
    start = pl.multiple_of(part * height, 16)
    w_grad = mm(left_ref[pl.ds(start, height)], lifted_grad).astype(bf16)
    for block in range(blocks):
        part_ref[block * height : (block + 1) * height] = w_grad[:, block * width : (block + 1) * width]
    out_grad = mm(left_ref[pl.ds(pl.multiple_of(features + start, 16), height)], cot).astype(bf16)
    part_ref[blocks * height : (blocks + 1) * height] = out_grad
    filled = (blocks + 1) * height
    if filled < part_ref.shape[0]:
        part_ref[filled:] = jnp.zeros((part_ref.shape[0] - filled, width), bf16)


def part_held(twist, group, replicas, back=0):
    half = lax.axis_index("shard") // group
    return lax.rem(lax.axis_index("replica") + half * twist + (replicas - back), replicas)


def layer_kernel(
    twist,
    group,
    small_ref,
    token_ref,
    same_ref,
    rows_ref,
    cot_ref,
    w_ref,
    wo_ref,
    lifted_ref,
    normal_ref,
    gate_ref,
    left_ref,
    *part_refs,
):
    replicas = len(part_refs) + 1
    tokens, width = rows_ref.shape
    head = width // HEADS
    embedded = mm(token_ref[...], rows_ref[...])
    same = jnp.concatenate([same_ref[...]] * HEADS, axis=0)

    lane = iota((1, width), 1)
    heads = [((lane >= h * head) & (lane < (h + 1) * head)).astype(f32) for h in range(HEADS)]

    def by_head(values):
        return jnp.concatenate([values * mask for mask in heads], axis=0).astype(bf16)

    def beside(values):
        return jnp.concatenate(
            [values[h * tokens : (h + 1) * tokens] for h in range(HEADS)], axis=1
        )

    norm_gain, gate_gain = small_ref[2:3, :width], small_ref[3:4, :width]
    normal, scale = center(embedded)
    scaled = normal * norm_gain
    normed = scaled.astype(bf16)
    left_ref[:width] = scaled.T.astype(bf16)
    lifted = mm(normed, w_ref[...])
    sig = sigmoid(lifted)
    projected = lifted * sig
    slope = sig * (1.0 + lifted * (1.0 - sig))
    gate_u = projected[:, :width]
    values = projected[:, width : 2 * width].astype(bf16).astype(f32)
    queries = projected[:, 2 * width : 3 * width].astype(bf16).astype(f32)
    keys = projected[:, 3 * width :].astype(bf16).astype(f32)

    queries_by, keys_by, values_by = by_head(queries), by_head(keys), by_head(values)
    scores = mm(queries_by, keys, (1, 1)) * head ** (-0.5)
    score_sig = sigmoid(scores)
    weights = (same * (scores * score_sig / MAXLEN)).astype(bf16)
    attended = mm(beside(weights), values_by)
    normal_two, scale_two = center(attended)
    left_ref[width:] = (normal_two * gate_gain * gate_u).T.astype(bf16)

    cot = cot_ref[...]
    gated_grad = mm(cot, wo_ref[...], (1, 1)).astype(bf16).astype(f32)
    normal_u = normal_two * gate_u
    gate_ref[...] = jnp.sum(gated_grad * normal_u, axis=0, keepdims=True)
    gated_gain = gated_grad * gate_gain
    u_grad = gated_gain * normal_two
    attended_grad = center_grad(gated_gain * gate_u, normal_two, scale_two)
    attended_by = by_head(attended_grad)
    weights_grad = mm(attended_by, values, (1, 1)).astype(bf16).astype(f32)
    values_grad = mm(weights, attended_by, (0, 0)).astype(bf16).astype(f32)
    score_slope = score_sig * (1.0 + scores * (1.0 - score_sig))
    scores_grad = (same * weights_grad * score_slope * (head ** (-0.5) / MAXLEN)).astype(bf16)
    queries_grad = mm(beside(scores_grad), keys_by).astype(bf16).astype(f32)
    keys_grad = mm(scores_grad, queries_by, (0, 0)).astype(bf16).astype(f32)
    lifted_grad = (
        jnp.concatenate([u_grad, values_grad, queries_grad, keys_grad], axis=1) * slope
    ).astype(bf16)
    lifted_ref[...] = lifted_grad
    normal_ref[:, :width] = normal
    normal_ref[:, width:] = jnp.broadcast_to(scale, (tokens, normal_ref.shape[1] - width))
    for step, part_ref in enumerate(part_refs, 1):
        part = part_held(twist, group, replicas, replicas - step)
        part_of_grads(part, width // replicas, left_ref, lifted_grad, cot, part_ref)


def finish_kernel(
    twist,
    group,
    replicas,
    small_ref,
    cot_ref,
    w_ref,
    lifted_ref,
    normal_ref,
    gate_ref,
    left_ref,
    slot_grad_ref,
    gain_ref,
    part_ref,
):
    tokens, width = cot_ref.shape
    part = part_held(twist, group, replicas)
    part_of_grads(part, width // replicas, left_ref, lifted_ref[...], cot_ref[...], part_ref)
    normal = normal_ref[:, :width]
    scale = normal_ref[:, width : width + 1]
    normed_grad = mm(lifted_ref[...], w_ref[...], (1, 1)).astype(bf16).astype(f32)
    norm_gain_grad = jnp.sum(normed_grad * normal, axis=0, keepdims=True)
    token_grad = cot_ref[...].astype(f32) + center_grad(
        normed_grad * small_ref[2:3, :width], normal, scale
    )
    slot_row = small_ref[0:1, :tokens].astype(jnp.int32)
    to_slot = (slot_row == iota((tokens, tokens), 0)).astype(f32)
    grad_high = token_grad.astype(bf16).astype(f32)
    slot_grad_ref[...] = mm(
        jnp.concatenate([to_slot, to_slot], axis=1),
        jnp.concatenate([grad_high, token_grad - grad_high], axis=0),
    ).astype(bf16)
    gains = jnp.concatenate([norm_gain_grad, gate_ref[...]], axis=0)
    high = gains.astype(bf16).astype(f32)
    gain_ref[...] = jnp.concatenate([high, gains - high], axis=0)


def halves_down(values):
    lanes = values.shape[-1] // 2
    return jnp.concatenate([values[..., :lanes], values[..., lanes:]], axis=-2)


def halves_across(values):
    rows = values.shape[-2] // 2
    return jnp.concatenate([values[..., :rows, :], values[..., rows:, :]], axis=-1)


def pack_kernel(group, slot_grad_ref, gain_ref, *refs):
    part_refs, out_ref = refs[:-1], refs[-1]
    half_slots, width = slot_grad_ref.shape[0] // 2, slot_grad_ref.shape[1]
    total = part_refs[0][...].astype(f32)
    for part_ref in part_refs[1:]:
        total = total + part_ref[...].astype(f32)
    half = lax.axis_index("shard") // group

    def slots_of(which):
        rows = pl.ds(pl.multiple_of(which * half_slots, 16), half_slots)
        return halves_down(slot_grad_ref[rows].astype(f32).reshape(group, -1, width))

    gains = halves_down(gain_ref[...])
    out_ref[...] = jnp.concatenate(
        [
            slots_of(half),
            slots_of(1 - half),
            halves_down(total.reshape(group, -1, width)),
            jnp.broadcast_to(gains[None], (group,) + gains.shape),
        ],
        axis=1,
    ).astype(bf16)


def as_two(values):
    high = values.astype(bf16).astype(f32)
    return jnp.concatenate([high, values - high], axis=0)


def cross_kernel(capacity, in_ref, cross_ref, theirs_ref, mine_ref):
    group, _, lanes = in_ref.shape
    slots = 2 * capacity
    mine_ref[...] = halves_across(in_ref[:, :slots].astype(f32)).reshape(mine_ref.shape).astype(bf16)
    theirs = halves_across(in_ref[:, slots : 2 * slots].astype(f32)).reshape(mine_ref.shape)
    total = in_ref[0, 2 * slots :].astype(f32)
    for peer in range(1, group):
        total = total + in_ref[peer, 2 * slots :].astype(f32)
    gains = halves_across(total[-GAIN_ROWS:])
    gains = as_two(gains[:2] + gains[2:])
    padding = jnp.zeros((GAIN_ROWS - gains.shape[0], 2 * lanes), f32)
    cross_ref[...] = halves_across(total[:-GAIN_ROWS]).astype(bf16)
    theirs_ref[...] = jnp.concatenate([theirs, gains, padding], axis=0).astype(bf16)


def share_kernel(grad_scale, mine_ref, other_ref, share_ref):
    group, _, _ = share_ref.shape
    total = mine_ref[...].astype(f32) + other_ref[...].astype(f32)
    share = (total * grad_scale).astype(bf16)
    for peer in range(group):
        share_ref[peer] = share


def slots_kernel(group, grad_scale, slots_ref, theirs_ref, other_ref, owned_ref):
    rows = slots_ref.shape[0]
    half = lax.axis_index("shard") // group
    owned_ref[pl.ds(pl.multiple_of(half * rows, 16), rows)] = slots_ref[...]
    owned_ref[pl.ds(pl.multiple_of((1 - half) * rows, 16), rows)] = other_ref[:rows]
    gains = theirs_ref[-GAIN_ROWS:].astype(f32) + other_ref[-GAIN_ROWS:].astype(f32)
    gains = as_two((gains[:2] + gains[2:4]) * grad_scale)
    padding = jnp.zeros((GAIN_ROWS - gains.shape[0], gains.shape[1]), f32)
    owned_ref[2 * rows :] = jnp.concatenate([gains, padding], axis=0).astype(bf16)


def adagrad_kernel(twist, group, replicas, *refs):
    wanted_refs, grad_refs = refs[:replicas], refs[replicas : 2 * replicas]
    state_ref, update_ref, state_out_ref, gains_ref = refs[2 * replicas :]
    rows = update_ref.shape[0]
    chunks, _, lanes = state_ref.shape
    slots = wanted_refs[0].shape[1]
    first = pl.program_id(0) * rows
    eye = iota((lanes, lanes), 0) == iota((lanes, lanes), 1)
    state = jnp.concatenate(
        [
            jnp.sum(jnp.where(eye, state_ref[chunk], 0.0), axis=1, keepdims=True)
            for chunk in range(chunks)
        ],
        axis=0,
    )
    delta = jnp.zeros(update_ref.shape, f32)
    squares = jnp.zeros((rows, 1), f32)
    gains = jnp.zeros((grad_refs[0].shape[0] - slots, update_ref.shape[1]), f32)
    wanted = [wanted_ref[...] for wanted_ref in wanted_refs]
    grads = [grad_ref[:slots].astype(f32) for grad_ref in grad_refs]
    if twist:
        start = lax.axis_index("shard") // group * (slots // 2)
        lane, row = iota((1, slots), 1), iota((slots, 1), 0)
        here = (lane >= start) & (lane < start + slots // 2)
        wanted = [jnp.where(here, *wanted), jnp.where(here, *wanted[::-1])]
        here = (row >= start) & (row < start + slots // 2)
        grads = [jnp.where(here, *grads), jnp.where(here, *grads[::-1])]
    for asked, grad, grad_ref in zip(wanted, grads, grad_refs):
        hit = iota((rows, slots), 0) + first == asked.astype(jnp.int32)
        row_grad = mm(hit.astype(f32), grad)
        mean_square = jnp.mean(row_grad * row_grad, axis=1, keepdims=True)
        delta = delta + row_grad * lax.rsqrt(state + mean_square + EPSILON)
        squares = squares + mean_square
        gains = gains + grad_ref[slots:].astype(f32)
    update_ref[...] = delta * (-LEARN_RATE / replicas)
    for chunk in range(chunks):
        column = squares[chunk * lanes : (chunk + 1) * lanes]
        square_row = jnp.sum(jnp.where(eye, column, 0.0), axis=0, keepdims=True)
        state_out_ref[chunk] = state_ref[chunk] + square_row / replicas
    gains_ref[...] = gains[:2] + gains[2:4]


def spread_kernel(twist, group, step, replicas, part_ref, *refs):
    uvqk_ref, out_ref, uvqk_rows, out_rows, sems = refs[-5:]
    height, columns = uvqk_rows.shape
    width = out_rows.shape[1]
    part = part_held(twist, group, replicas, step)
    rows = pl.ds(pl.multiple_of(part * height, 8), height)
    blocks = columns // width
    for block in range(blocks):
        uvqk_rows[:, block * width : (block + 1) * width] = part_ref[
            block * height : (block + 1) * height
        ].astype(f32)
    first = pltpu.make_async_copy(uvqk_rows, uvqk_ref.at[rows], sems.at[0])
    first.start()
    out_rows[...] = part_ref[blocks * height : (blocks + 1) * height].astype(f32)
    second = pltpu.make_async_copy(out_rows, out_ref.at[rows], sems.at[1])
    second.start()
    first.wait()
    second.wait()


def hand_on(parts):
    replicas = len(parts)
    came = [parts[0]]
    for step in range(1, replicas):
        pairs = [(source, (source + step) % replicas) for source in range(replicas)]
        came.append(lax.ppermute(parts[step], "replica", pairs))
    return came


def from_all(value, replicas):
    came = hand_on([value] * replicas)
    if replicas > 2:
        order = lax.rem(lax.axis_index("replica") - jnp.arange(replicas) + replicas, replicas)
        stacked = jnp.take(jnp.stack(came), order, axis=0)
        came = [stacked[index] for index in range(replicas)]
    return came


def on_device(
    request_rows,
    token_slot,
    seq_lengths,
    cotangent,
    table_slab,
    adagrad_state,
    w_uvqk,
    w_out,
    norm_gain,
    out_gain,
):
    shards = lax.axis_size("shard")
    replicas = lax.axis_size("replica")
    tokens = token_slot.shape[1]
    rows_dev, width = table_slab.shape
    capacity = tokens // shards
    blocks = w_uvqk.shape[1] // width + 1
    group = shards // 2
    share_rows = -(-blocks * width // (replicas * group))
    part_rows = share_rows * group
    in_half = [list(range(group)), list(range(group, shards))]
    twist = 1 if replicas == 2 else 0
    both = ("shard", "replica")
    place = lambda replica, shard: shard * replicas + replica % replicas
    lookup_groups = [
        [place(replica + shard // group * twist, shard) for shard in range(shards)]
        for replica in range(replicas)
    ]
    half_slots = group * capacity
    grad_scale = 1.0 / math.sqrt(tokens * shards * replicas)
    shape = jax.ShapeDtypeStruct

    asked, small = pl.pallas_call(
        ready_kernel,
        out_shape=(
            shape((shards, 1, tokens), jnp.int32),
            shape((8, max(width, tokens)), f32),
        ),
        in_specs=[VMEM] * 5,
        out_specs=(VMEM, VMEM),
        cost_estimate=estimate(rows_dev * width * 8192, rows_dev * width * 128),
        compiler_params=room(4),
        name="ready",
    )(
        request_rows,
        token_slot,
        seq_lengths.reshape(1, -1),
        norm_gain.reshape(1, width),
        out_gain.reshape(1, width),
    )
    ids = lax.all_to_all(
        asked, both, split_axis=0, concat_axis=0, tiled=True, axis_index_groups=lookup_groups
    )
    found, wanted, token_hot, same = pl.pallas_call(
        functools.partial(fetch_kernel, capacity, seq_lengths.shape[-1]),
        out_shape=(
            shape((tokens, width), bf16),
            shape((1, tokens), f32),
            shape((tokens, tokens), bf16),
            shape((tokens, tokens), f32),
        ),
        in_specs=[VMEM] * 3,
        out_specs=(VMEM,) * 4,
        cost_estimate=estimate(2 * tokens * rows_dev * width, rows_dev * width * 4),
        compiler_params=room(8),
        name="fetch",
    )(ids, table_slab, small)
    slot_rows = lax.all_to_all(
        found.reshape(shards, capacity, width),
        both,
        split_axis=0,
        concat_axis=0,
        tiled=True,
        axis_index_groups=lookup_groups,
    ).reshape(tokens, width)

    cot = cotangent.reshape(tokens, width)
    lifted_grad, normal, gate_grad, left, *parts = pl.pallas_call(
        functools.partial(layer_kernel, 0, group),
        out_shape=(
            shape((tokens, w_uvqk.shape[1]), bf16),
            shape((tokens, width + 128), f32),
            shape((1, width), f32),
            shape((2 * width, tokens), bf16),
        )
        + (shape((part_rows, width), bf16),) * (replicas - 1),
        in_specs=[VMEM] * 7,
        out_specs=(VMEM,) * (replicas + 3),
        cost_estimate=estimate(8 * tokens * width * w_uvqk.shape[1], 4 * blocks * width * width),
        compiler_params=room(20),
        name="layer",
    )(small, token_hot, same, slot_rows, cot, w_uvqk, w_out)
    came = hand_on([None] + parts)[1:]
    slot_grad, gain_rows, kept = pl.pallas_call(
        functools.partial(finish_kernel, 0, group, replicas),
        out_shape=(
            shape((tokens, width), bf16),
            shape((4, width), f32),
            shape((part_rows, width), bf16),
        ),
        in_specs=[VMEM] * 7,
        out_specs=(VMEM,) * 3,
        cost_estimate=estimate(3 * tokens * width * w_uvqk.shape[1], 3 * blocks * width * width),
        compiler_params=room(10),
        name="finish",
    )(small, cot, w_uvqk, lifted_grad, normal, gate_grad, left)
    came = [kept] + came

    aligned = capacity % 8 == 0 and share_rows % 8 == 0
    message_rows = 2 * (2 * capacity + share_rows) + GAIN_ROWS
    if aligned:
        message = pl.pallas_call(
            functools.partial(pack_kernel, group),
            out_shape=shape((group, message_rows, width // 2), bf16),
            in_specs=[VMEM] * (replicas + 2),
            out_specs=VMEM,
            compiler_params=room(10),
            name="pack",
        )(slot_grad, gain_rows, *came)
    else:
        half = lax.axis_index("shard") // group
        by_half = slot_grad.reshape(2, group, capacity, width)
        total = sum(part.astype(f32) for part in came).astype(bf16)
        message = jnp.concatenate(
            [
                jnp.take(by_half, half, axis=0),
                jnp.take(by_half, 1 - half, axis=0),
                total.reshape(group, share_rows, width),
                jnp.broadcast_to(gain_rows.astype(bf16)[None], (group, 4, width)),
            ],
            axis=1,
        )
    arrived = lax.all_to_all(
        message, "shard", split_axis=0, concat_axis=0, tiled=True, axis_index_groups=in_half
    )
    if aligned:
        cross, theirs, mine = pl.pallas_call(
            functools.partial(cross_kernel, capacity),
            out_shape=(
                shape((share_rows, width), bf16),
                shape((half_slots + GAIN_ROWS, width), bf16),
                shape((half_slots, width), bf16),
            ),
            in_specs=[VMEM],
            out_specs=(VMEM,) * 3,
            compiler_params=room(8),
            name="cross",
        )(arrived)
    else:
        mine = arrived[:, :capacity].reshape(half_slots, width)
        theirs = arrived[:, capacity : 2 * capacity].reshape(half_slots, width)
        total = jnp.sum(arrived[:, 2 * capacity :].astype(f32), axis=0)
        gains = as_two(total[share_rows : share_rows + 2] + total[share_rows + 2 :]).astype(bf16)
        padding = jnp.zeros((GAIN_ROWS - 4, width), bf16)
        cross = total[:share_rows].astype(bf16)
        theirs = jnp.concatenate([theirs, gains, padding], axis=0)
    mirror = [(shard, (shard + group) % shards) for shard in range(shards)]
    turned_mirror = [
        (place(replica, shard), place(replica + twist, (shard + group) % shards))
        for replica in range(replicas)
        for shard in range(shards)
    ]
    other = lax.ppermute(cross, "shard", mirror)
    other_slots = lax.ppermute(theirs, both, turned_mirror)
    if aligned:
        share = pl.pallas_call(
            functools.partial(share_kernel, grad_scale),
            out_shape=shape((group, share_rows, width), bf16),
            in_specs=[VMEM] * 2,
            out_specs=VMEM,
            compiler_params=room(4),
            name="share",
        )(cross, other)
        owned = pl.pallas_call(
            functools.partial(slots_kernel, group, grad_scale),
            out_shape=shape((tokens + GAIN_ROWS, width), bf16),
            in_specs=[VMEM] * 3,
            out_specs=VMEM,
            cost_estimate=estimate(tokens * width, 4 * tokens * width),
            compiler_params=room(4),
            name="slots",
        )(mine, theirs, other_slots)
    else:
        total = (cross.astype(f32) + other.astype(f32)) * grad_scale
        share = jnp.broadcast_to(total.astype(bf16)[None], (group, share_rows, width))
        gains = theirs[half_slots:].astype(f32) + other_slots[half_slots:].astype(f32)
        gains = as_two((gains[:2] + gains[2:4]) * grad_scale)
        by_half = jnp.stack([mine, other_slots[:half_slots]])
        by_half = jnp.where(half == 0, by_half, by_half[::-1]).reshape(tokens, width)
        owned = jnp.concatenate([by_half, gains.astype(bf16), padding], axis=0)

    gathered = lax.all_to_all(
        share, "shard", split_axis=0, concat_axis=0, tiled=True, axis_index_groups=in_half
    )

    wanted_all = from_all(wanted, replicas)
    owned_all = from_all(owned, replicas)
    lanes = 128
    block = min(rows_dev, 2048 // replicas)
    row_update, state_new, grad_gains = pl.pallas_call(
        functools.partial(adagrad_kernel, twist, group, replicas),
        grid=(rows_dev // block,),
        out_shape=(
            shape((rows_dev, width), f32),
            shape((rows_dev // lanes, 1, lanes), f32),
            shape((2, width), f32),
        ),
        in_specs=[pl.BlockSpec((1, tokens), lambda step: (0, 0))] * replicas
        + [pl.BlockSpec((tokens + GAIN_ROWS, width), lambda step: (0, 0))] * replicas
        + [pl.BlockSpec((block // lanes, 1, lanes), lambda step: (step, 0, 0))],
        out_specs=(
            pl.BlockSpec((block, width), lambda step: (step, 0)),
            pl.BlockSpec((block // lanes, 1, lanes), lambda step: (step, 0, 0)),
            pl.BlockSpec((2, width), lambda step: (0, 0)),
        ),
        cost_estimate=estimate(2 * replicas * tokens * rows_dev * width, rows_dev * width * 4),
        compiler_params=room(12),
        name="adagrad",
    )(*wanted_all, *owned_all, adagrad_state.reshape(rows_dev // lanes, 1, lanes))

    halves = hand_on([gathered.reshape(part_rows, width)] * replicas)
    grads = ()
    for step, half in enumerate(halves):
        grads = pl.pallas_call(
            functools.partial(spread_kernel, 0, group, step, replicas),
            out_shape=(shape(w_uvqk.shape, f32), shape(w_out.shape, f32)),
            in_specs=[VMEM] + [pl.BlockSpec(memory_space=pl.ANY)] * len(grads),
            out_specs=(pl.BlockSpec(memory_space=pl.ANY),) * 2,
            scratch_shapes=[
                pltpu.VMEM((width // replicas, w_uvqk.shape[1]), f32),
                pltpu.VMEM((width // replicas, width), f32),
                pltpu.SemaphoreType.DMA((2,)),
            ],
            input_output_aliases={1: 0, 2: 1} if grads else {},
            cost_estimate=estimate(blocks * width * width, 3 * blocks * width * width),
            compiler_params=room(6),
        )(half, *grads)
    return (row_update, state_new.reshape(rows_dev), *grads, grad_gains)


def solution(mesh):
    placed = (
        P("replica", "shard", None),
        P("replica", "shard"),
        P("replica", "shard", None),
        P("replica", "shard", None),
        P("shard", None),
        P("shard"),
        P(),
        P(),
        P(),
        P(),
    )

    return jax.shard_map(
        on_device,
        mesh=mesh,
        in_specs=placed,
        out_specs=(P("shard", None), P("shard"), P(), P(), P()),
        check_vma=False,
    )
```

```python
import functools
import math

import jax
import jax.numpy as jnp
from jax import lax
from jax.experimental import pallas as pl
from jax.experimental.pallas import tpu as pltpu
from jax.sharding import PartitionSpec as P


HEADS = 4
MAXLEN = 48
EPSILON = 1e-08
LEARN_RATE = 0.5
NORM_EPSILON = 1e-05
GAIN_ROWS = 8

f32 = jnp.float32
bf16 = jnp.bfloat16
VMEM = pl.BlockSpec(memory_space=pltpu.VMEM)


def room(mebibytes):
    return pltpu.CompilerParams(vmem_limit_bytes=mebibytes * 2**20)


def iota(shape, axis):
    return lax.broadcasted_iota(jnp.int32, shape, axis)


def mm(left, right, contract=(1, 0)):
    return lax.dot_general(
        left.astype(bf16),
        right.astype(bf16),
        (((contract[0],), (contract[1],)), ((), ())),
        preferred_element_type=f32,
    )


def estimate(flops, bytes_accessed):
    return pl.CostEstimate(flops=flops, bytes_accessed=bytes_accessed, transcendentals=0)


def ready_kernel(asked_ref, slot_ref, length_ref, norm_ref, gate_ref, ids_ref, small_ref):
    ids_ref[...] = jnp.broadcast_to(asked_ref[...], ids_ref.shape)
    small_ref[0:1, : slot_ref.shape[1]] = slot_ref[...].astype(f32)
    small_ref[1:2, : length_ref.shape[1]] = length_ref[...].astype(f32)
    small_ref[2:3, : norm_ref.shape[1]] = norm_ref[...]
    small_ref[3:4, : gate_ref.shape[1]] = gate_ref[...]


def segments(lengths):
    count = lengths.shape[1]
    row, col = iota((count, count), 0), iota((count, count), 1)
    column = jnp.sum(jnp.where(row == col, lengths, 0.0), axis=1, keepdims=True)
    ends_column = jnp.sum(jnp.where(col <= row, lengths, 0.0), axis=1, keepdims=True)
    ends_row = jnp.sum(jnp.where(row <= col, column, 0.0), axis=0, keepdims=True)
    return ends_row, ends_column


def token_kernel(histories, small_ref, token_ref, same_ref):
    tokens = token_ref.shape[0]
    row, col = iota((tokens, tokens), 0), iota((tokens, tokens), 1)
    slot_row = small_ref[0:1, :tokens]
    slot_column = jnp.sum(jnp.where(row == col, slot_row, 0.0), axis=1, keepdims=True)
    token_ref[...] = (slot_column.astype(jnp.int32) == col).astype(f32).astype(bf16)
    ends_row, ends_column = segments(small_ref[1:2, :histories])
    before_row = iota((histories, tokens), 1).astype(f32) >= ends_column
    segment_row = jnp.sum(before_row.astype(f32), axis=0, keepdims=True)
    before_column = iota((tokens, histories), 0).astype(f32) >= ends_row
    segment_column = jnp.sum(before_column.astype(f32), axis=1, keepdims=True)
    same_ref[...] = ((segment_row == segment_column) & (row >= col)).astype(f32)


def fetch_kernel(
    capacity, histories, ids_ref, table_ref, small_ref, found_ref, wanted_ref, token_ref, same_ref
):
    token_kernel(histories, small_ref, token_ref, same_ref)
    me = lax.axis_index("shard")
    ids = ids_ref[...].reshape(ids_ref.shape[0], ids_ref.shape[2])
    shards, slots = ids.shape
    rows = table_ref.shape[0]
    high = (ids >> 5).astype(f32)
    low = (ids & 31).astype(f32)
    slot = iota((slots, shards), 0)
    first = iota((slots, shards), 1) * capacity
    expand = ((slot >= first) & (slot < first + capacity)).astype(f32)
    asked = mm(expand, high) * 32.0 + mm(expand, low)
    pick = iota((slots, slots), 1) == me * capacity + lax.rem(iota((slots, slots), 0), capacity)
    column = jnp.sum(jnp.where(pick, asked, 0.0), axis=1, keepdims=True)
    eye = iota((slots, slots), 0) == iota((slots, slots), 1)
    wanted_ref[...] = jnp.sum(jnp.where(eye, column, 0.0), axis=0, keepdims=True)
    chosen = (column.astype(jnp.int32) == iota((slots, rows), 1)).astype(f32)
    found_ref[...] = mm(chosen, table_ref[...]).astype(bf16)


def center(values):
    shifted = values - jnp.mean(values, axis=1, keepdims=True)
    scale = lax.rsqrt(jnp.mean(shifted * shifted, axis=1, keepdims=True) + NORM_EPSILON)
    return shifted * scale, scale


def center_grad(grad, normal, scale):
    along = jnp.mean(grad * normal, axis=1, keepdims=True)
    return scale * (grad - jnp.mean(grad, axis=1, keepdims=True) - normal * along)


def sigmoid(values):
    return 0.5 + 0.5 * jnp.tanh(0.5 * values)


def part_of_grads(part, height, left_ref, lifted_grad, cot, part_ref):
    width = cot.shape[1]
    blocks = lifted_grad.shape[1] // width
    features = left_ref.shape[0] // 2
    start = pl.multiple_of(part * height, 16)
    w_grad = mm(left_ref[pl.ds(start, height)], lifted_grad).astype(bf16)
    for block in range(blocks):
        part_ref[block * height : (block + 1) * height] = w_grad[:, block * width : (block + 1) * width]
    out_grad = mm(left_ref[pl.ds(pl.multiple_of(features + start, 16), height)], cot).astype(bf16)
    part_ref[blocks * height : (blocks + 1) * height] = out_grad
    filled = (blocks + 1) * height
    if filled < part_ref.shape[0]:
        part_ref[filled:] = jnp.zeros((part_ref.shape[0] - filled, width), bf16)


def part_held(twist, group, replicas, back=0):
    odd = lax.rem(lax.axis_index("shard") * 2 // group, 2)
    return lax.rem(lax.axis_index("replica") + odd * twist + (replicas - back), replicas)


def layer_kernel(
    twist,
    group,
    small_ref,
    token_ref,
    same_ref,
    rows_ref,
    cot_ref,
    w_ref,
    wo_ref,
    lifted_ref,
    normal_ref,
    gate_ref,
    left_ref,
    *part_refs,
):
    replicas = len(part_refs) + 1
    tokens, width = rows_ref.shape
    head = width // HEADS
    embedded = mm(token_ref[...], rows_ref[...])
    same = jnp.concatenate([same_ref[...]] * HEADS, axis=0)

    lane = iota((1, width), 1)
    heads = [((lane >= h * head) & (lane < (h + 1) * head)).astype(f32) for h in range(HEADS)]

    def by_head(values):
        return jnp.concatenate([values * mask for mask in heads], axis=0).astype(bf16)

    def beside(values):
        return jnp.concatenate(
            [values[h * tokens : (h + 1) * tokens] for h in range(HEADS)], axis=1
        )

    norm_gain, gate_gain = small_ref[2:3, :width], small_ref[3:4, :width]
    normal, scale = center(embedded)
    scaled = normal * norm_gain
    normed = scaled.astype(bf16)
    left_ref[:width] = scaled.T.astype(bf16)
    lifted = mm(normed, w_ref[...])
    sig = sigmoid(lifted)
    projected = lifted * sig
    slope = sig * (1.0 + lifted * (1.0 - sig))
    gate_u = projected[:, :width]
    values = projected[:, width : 2 * width].astype(bf16).astype(f32)
    queries = projected[:, 2 * width : 3 * width].astype(bf16).astype(f32)
    keys = projected[:, 3 * width :].astype(bf16).astype(f32)

    queries_by, keys_by, values_by = by_head(queries), by_head(keys), by_head(values)
    scores = mm(queries_by, keys, (1, 1)) * head ** (-0.5)
    score_sig = sigmoid(scores)
    weights = (same * (scores * score_sig / MAXLEN)).astype(bf16)
    attended = mm(beside(weights), values_by)
    normal_two, scale_two = center(attended)
    left_ref[width:] = (normal_two * gate_gain * gate_u).T.astype(bf16)

    cot = cot_ref[...]
    gated_grad = mm(cot, wo_ref[...], (1, 1)).astype(bf16).astype(f32)
    normal_u = normal_two * gate_u
    gate_ref[...] = jnp.sum(gated_grad * normal_u, axis=0, keepdims=True)
    gated_gain = gated_grad * gate_gain
    u_grad = gated_gain * normal_two
    attended_grad = center_grad(gated_gain * gate_u, normal_two, scale_two)
    attended_by = by_head(attended_grad)
    weights_grad = mm(attended_by, values, (1, 1)).astype(bf16).astype(f32)
    values_grad = mm(weights, attended_by, (0, 0)).astype(bf16).astype(f32)
    score_slope = score_sig * (1.0 + scores * (1.0 - score_sig))
    scores_grad = (same * weights_grad * score_slope * (head ** (-0.5) / MAXLEN)).astype(bf16)
    queries_grad = mm(beside(scores_grad), keys_by).astype(bf16).astype(f32)
    keys_grad = mm(scores_grad, queries_by, (0, 0)).astype(bf16).astype(f32)
    lifted_grad = (
        jnp.concatenate([u_grad, values_grad, queries_grad, keys_grad], axis=1) * slope
    ).astype(bf16)
    lifted_ref[...] = lifted_grad
    normal_ref[:, :width] = normal
    normal_ref[:, width:] = jnp.broadcast_to(scale, (tokens, normal_ref.shape[1] - width))
    for step, part_ref in enumerate(part_refs, 1):
        part = part_held(twist, group, replicas, replicas - step)
        part_of_grads(part, width // replicas, left_ref, lifted_grad, cot, part_ref)


def finish_kernel(
    twist,
    group,
    replicas,
    small_ref,
    cot_ref,
    w_ref,
    lifted_ref,
    normal_ref,
    gate_ref,
    left_ref,
    slot_grad_ref,
    gain_ref,
    part_ref,
):
    tokens, width = cot_ref.shape
    part = part_held(twist, group, replicas)
    part_of_grads(part, width // replicas, left_ref, lifted_ref[...], cot_ref[...], part_ref)
    normal = normal_ref[:, :width]
    scale = normal_ref[:, width : width + 1]
    normed_grad = mm(lifted_ref[...], w_ref[...], (1, 1)).astype(bf16).astype(f32)
    norm_gain_grad = jnp.sum(normed_grad * normal, axis=0, keepdims=True)
    token_grad = cot_ref[...].astype(f32) + center_grad(
        normed_grad * small_ref[2:3, :width], normal, scale
    )
    slot_row = small_ref[0:1, :tokens].astype(jnp.int32)
    to_slot = (slot_row == iota((tokens, tokens), 0)).astype(f32)
    grad_high = token_grad.astype(bf16).astype(f32)
    slot_grad_ref[...] = mm(
        jnp.concatenate([to_slot, to_slot], axis=1),
        jnp.concatenate([grad_high, token_grad - grad_high], axis=0),
    ).astype(bf16)
    gains = jnp.concatenate([norm_gain_grad, gate_ref[...]], axis=0)
    high = gains.astype(bf16).astype(f32)
    gain_ref[...] = jnp.concatenate([high, gains - high], axis=0)


def halves_down(values):
    lanes = values.shape[-1] // 2
    return jnp.concatenate([values[..., :lanes], values[..., lanes:]], axis=-2)


def halves_across(values):
    rows = values.shape[-2] // 2
    return jnp.concatenate([values[..., :rows, :], values[..., rows:, :]], axis=-1)


def pack_kernel(group, slot_grad_ref, gain_ref, *refs):
    part_refs, out_ref = refs[:-1], refs[-1]
    half_slots, width = slot_grad_ref.shape[0] // 2, slot_grad_ref.shape[1]
    total = part_refs[0][...].astype(f32)
    for part_ref in part_refs[1:]:
        total = total + part_ref[...].astype(f32)
    half = lax.axis_index("shard") // group

    def slots_of(which):
        rows = pl.ds(pl.multiple_of(which * half_slots, 16), half_slots)
        return halves_down(slot_grad_ref[rows].astype(f32).reshape(group, -1, width))

    gains = halves_down(gain_ref[...])
    out_ref[...] = jnp.concatenate(
        [
            slots_of(half),
            slots_of(1 - half),
            halves_down(total.reshape(group, -1, width)),
            jnp.broadcast_to(gains[None], (group,) + gains.shape),
        ],
        axis=1,
    ).astype(bf16)


def as_two(values):
    high = values.astype(bf16).astype(f32)
    return jnp.concatenate([high, values - high], axis=0)


def cross_kernel(capacity, in_ref, cross_ref, theirs_ref, mine_ref):
    group, _, lanes = in_ref.shape
    slots = 2 * capacity
    mine_ref[...] = halves_across(in_ref[:, :slots].astype(f32)).reshape(mine_ref.shape).astype(bf16)
    theirs = halves_across(in_ref[:, slots : 2 * slots].astype(f32)).reshape(mine_ref.shape)
    total = in_ref[0, 2 * slots :].astype(f32)
    for peer in range(1, group):
        total = total + in_ref[peer, 2 * slots :].astype(f32)
    gains = halves_across(total[-GAIN_ROWS:])
    gains = as_two(gains[:2] + gains[2:])
    padding = jnp.zeros((GAIN_ROWS - gains.shape[0], 2 * lanes), f32)
    cross_ref[...] = halves_across(total[:-GAIN_ROWS]).astype(bf16)
    theirs_ref[...] = jnp.concatenate([theirs, gains, padding], axis=0).astype(bf16)


def share_kernel(grad_scale, mine_ref, other_ref, share_ref):
    group, _, _ = share_ref.shape
    total = mine_ref[...].astype(f32) + other_ref[...].astype(f32)
    share = (total * grad_scale).astype(bf16)
    for peer in range(group):
        share_ref[peer] = share


def slots_kernel(group, grad_scale, slots_ref, theirs_ref, other_ref, owned_ref):
    rows = slots_ref.shape[0]
    half = lax.axis_index("shard") // group
    owned_ref[pl.ds(pl.multiple_of(half * rows, 16), rows)] = slots_ref[...]
    owned_ref[pl.ds(pl.multiple_of((1 - half) * rows, 16), rows)] = other_ref[:rows]
    gains = theirs_ref[-GAIN_ROWS:].astype(f32) + other_ref[-GAIN_ROWS:].astype(f32)
    gains = as_two((gains[:2] + gains[2:4]) * grad_scale)
    padding = jnp.zeros((GAIN_ROWS - gains.shape[0], gains.shape[1]), f32)
    owned_ref[2 * rows :] = jnp.concatenate([gains, padding], axis=0).astype(bf16)


def adagrad_kernel(twist, replicas, *refs):
    wanted_refs, grad_refs = refs[:replicas], refs[replicas : 2 * replicas]
    state_ref, update_ref, state_out_ref, gains_ref = refs[2 * replicas :]
    rows = update_ref.shape[0]
    chunks, _, lanes = state_ref.shape
    slots = wanted_refs[0].shape[1]
    first = pl.program_id(0) * rows
    eye = iota((lanes, lanes), 0) == iota((lanes, lanes), 1)
    state = jnp.concatenate(
        [
            jnp.sum(jnp.where(eye, state_ref[chunk], 0.0), axis=1, keepdims=True)
            for chunk in range(chunks)
        ],
        axis=0,
    )
    delta = jnp.zeros(update_ref.shape, f32)
    squares = jnp.zeros((rows, 1), f32)
    gains = jnp.zeros((grad_refs[0].shape[0] - slots, update_ref.shape[1]), f32)
    wanted = [wanted_ref[...] for wanted_ref in wanted_refs]
    grads = [grad_ref[:slots].astype(f32) for grad_ref in grad_refs]
    if twist:
        def even(index):
            quarter = slots // 4
            return (index < quarter) | ((index >= 2 * quarter) & (index < 3 * quarter))

        here = even(iota((1, slots), 1))
        wanted = [jnp.where(here, *wanted), jnp.where(here, *wanted[::-1])]
        here = even(iota((slots, 1), 0))
        grads = [jnp.where(here, *grads), jnp.where(here, *grads[::-1])]
    for asked, grad, grad_ref in zip(wanted, grads, grad_refs):
        hit = iota((rows, slots), 0) + first == asked.astype(jnp.int32)
        row_grad = mm(hit.astype(f32), grad)
        mean_square = jnp.mean(row_grad * row_grad, axis=1, keepdims=True)
        delta = delta + row_grad * lax.rsqrt(state + mean_square + EPSILON)
        squares = squares + mean_square
        gains = gains + grad_ref[slots:].astype(f32)
    update_ref[...] = delta * (-LEARN_RATE / replicas)
    for chunk in range(chunks):
        column = squares[chunk * lanes : (chunk + 1) * lanes]
        square_row = jnp.sum(jnp.where(eye, column, 0.0), axis=0, keepdims=True)
        state_out_ref[chunk] = state_ref[chunk] + square_row / replicas
    gains_ref[...] = gains[:2] + gains[2:4]


def spread_kernel(twist, group, step, replicas, part_ref, *refs):
    uvqk_ref, out_ref, uvqk_rows, out_rows, sems = refs[-5:]
    height, columns = uvqk_rows.shape
    width = out_rows.shape[1]
    part = part_held(twist, group, replicas, step)
    rows = pl.ds(pl.multiple_of(part * height, 8), height)
    blocks = columns // width
    for block in range(blocks):
        uvqk_rows[:, block * width : (block + 1) * width] = part_ref[
            block * height : (block + 1) * height
        ].astype(f32)
    first = pltpu.make_async_copy(uvqk_rows, uvqk_ref.at[rows], sems.at[0])
    first.start()
    out_rows[...] = part_ref[blocks * height : (blocks + 1) * height].astype(f32)
    second = pltpu.make_async_copy(out_rows, out_ref.at[rows], sems.at[1])
    second.start()
    first.wait()
    second.wait()


def hand_on(parts):
    replicas = len(parts)
    came = [parts[0]]
    for step in range(1, replicas):
        pairs = [(source, (source + step) % replicas) for source in range(replicas)]
        came.append(lax.ppermute(parts[step], "replica", pairs))
    return came


def from_all(value, replicas):
    came = hand_on([value] * replicas)
    if replicas > 2:
        order = lax.rem(lax.axis_index("replica") - jnp.arange(replicas) + replicas, replicas)
        stacked = jnp.take(jnp.stack(came), order, axis=0)
        came = [stacked[index] for index in range(replicas)]
    return came


def on_device(
    request_rows,
    token_slot,
    seq_lengths,
    cotangent,
    table_slab,
    adagrad_state,
    w_uvqk,
    w_out,
    norm_gain,
    out_gain,
):
    shards = lax.axis_size("shard")
    replicas = lax.axis_size("replica")
    tokens = token_slot.shape[1]
    rows_dev, width = table_slab.shape
    capacity = tokens // shards
    blocks = w_uvqk.shape[1] // width + 1
    group = shards // 2
    share_rows = -(-blocks * width // (replicas * group))
    part_rows = share_rows * group
    twist = 1 if replicas == 2 and shards % 4 == 0 else 0
    both = ("shard", "replica")

    def members(replica, first, last):
        turned = [(replica + shard * 4 // shards * twist) % replicas for shard in range(first, last)]
        return [shard * replicas + turn for shard, turn in zip(range(first, last), turned)]

    lookup_groups = [members(replica, 0, shards) for replica in range(replicas)]
    half_groups = [
        members(replica, first, first + group) for replica in range(replicas) for first in (0, group)
    ]
    half_slots = group * capacity
    grad_scale = 1.0 / math.sqrt(tokens * shards * replicas)
    shape = jax.ShapeDtypeStruct

    asked, small = pl.pallas_call(
        ready_kernel,
        out_shape=(
            shape((shards, 1, tokens), jnp.int32),
            shape((8, max(width, tokens)), f32),
        ),
        in_specs=[VMEM] * 5,
        out_specs=(VMEM, VMEM),
        cost_estimate=estimate(rows_dev * width * 8192, rows_dev * width * 128),
        compiler_params=room(4),
        name="ready",
    )(
        request_rows,
        token_slot,
        seq_lengths.reshape(1, -1),
        norm_gain.reshape(1, width),
        out_gain.reshape(1, width),
    )
    ids = lax.all_to_all(
        asked, both, split_axis=0, concat_axis=0, tiled=True, axis_index_groups=lookup_groups
    )
    found, wanted, token_hot, same = pl.pallas_call(
        functools.partial(fetch_kernel, capacity, seq_lengths.shape[-1]),
        out_shape=(
            shape((tokens, width), bf16),
            shape((1, tokens), f32),
            shape((tokens, tokens), bf16),
            shape((tokens, tokens), f32),
        ),
        in_specs=[VMEM] * 3,
        out_specs=(VMEM,) * 4,
        cost_estimate=estimate(2 * tokens * rows_dev * width, rows_dev * width * 4),
        compiler_params=room(8),
        name="fetch",
    )(ids, table_slab, small)
    slot_rows = lax.all_to_all(
        found.reshape(shards, capacity, width),
        both,
        split_axis=0,
        concat_axis=0,
        tiled=True,
        axis_index_groups=lookup_groups,
    ).reshape(tokens, width)

    cot = cotangent.reshape(tokens, width)
    lifted_grad, normal, gate_grad, left, *parts = pl.pallas_call(
        functools.partial(layer_kernel, twist, group),
        out_shape=(
            shape((tokens, w_uvqk.shape[1]), bf16),
            shape((tokens, width + 128), f32),
            shape((1, width), f32),
            shape((2 * width, tokens), bf16),
        )
        + (shape((part_rows, width), bf16),) * (replicas - 1),
        in_specs=[VMEM] * 7,
        out_specs=(VMEM,) * (replicas + 3),
        cost_estimate=estimate(8 * tokens * width * w_uvqk.shape[1], 4 * blocks * width * width),
        compiler_params=room(20),
        name="layer",
    )(small, token_hot, same, slot_rows, cot, w_uvqk, w_out)
    came = hand_on([None] + parts)[1:]
    slot_grad, gain_rows, kept = pl.pallas_call(
        functools.partial(finish_kernel, twist, group, replicas),
        out_shape=(
            shape((tokens, width), bf16),
            shape((4, width), f32),
            shape((part_rows, width), bf16),
        ),
        in_specs=[VMEM] * 7,
        out_specs=(VMEM,) * 3,
        cost_estimate=estimate(3 * tokens * width * w_uvqk.shape[1], 3 * blocks * width * width),
        compiler_params=room(10),
        name="finish",
    )(small, cot, w_uvqk, lifted_grad, normal, gate_grad, left)
    came = [kept] + came

    aligned = capacity % 8 == 0 and share_rows % 8 == 0
    message_rows = 2 * (2 * capacity + share_rows) + GAIN_ROWS
    if aligned:
        message = pl.pallas_call(
            functools.partial(pack_kernel, group),
            out_shape=shape((group, message_rows, width // 2), bf16),
            in_specs=[VMEM] * (replicas + 2),
            out_specs=VMEM,
            compiler_params=room(10),
            name="pack",
        )(slot_grad, gain_rows, *came)
    else:
        half = lax.axis_index("shard") // group
        by_half = slot_grad.reshape(2, group, capacity, width)
        total = sum(part.astype(f32) for part in came).astype(bf16)
        message = jnp.concatenate(
            [
                jnp.take(by_half, half, axis=0),
                jnp.take(by_half, 1 - half, axis=0),
                total.reshape(group, share_rows, width),
                jnp.broadcast_to(gain_rows.astype(bf16)[None], (group, 4, width)),
            ],
            axis=1,
        )
    arrived = lax.all_to_all(
        message, both, split_axis=0, concat_axis=0, tiled=True, axis_index_groups=half_groups
    )
    if aligned:
        cross, theirs, mine = pl.pallas_call(
            functools.partial(cross_kernel, capacity),
            out_shape=(
                shape((share_rows, width), bf16),
                shape((half_slots + GAIN_ROWS, width), bf16),
                shape((half_slots, width), bf16),
            ),
            in_specs=[VMEM],
            out_specs=(VMEM,) * 3,
            compiler_params=room(8),
            name="cross",
        )(arrived)
    else:
        mine = arrived[:, :capacity].reshape(half_slots, width)
        theirs = arrived[:, capacity : 2 * capacity].reshape(half_slots, width)
        total = jnp.sum(arrived[:, 2 * capacity :].astype(f32), axis=0)
        gains = as_two(total[share_rows : share_rows + 2] + total[share_rows + 2 :]).astype(bf16)
        padding = jnp.zeros((GAIN_ROWS - 4, width), bf16)
        cross = total[:share_rows].astype(bf16)
        theirs = jnp.concatenate([theirs, gains, padding], axis=0)
    mirror = [(shard, (shard + group) % shards) for shard in range(shards)]
    other = lax.ppermute(cross, "shard", mirror)
    other_slots = lax.ppermute(theirs, "shard", mirror)
    if aligned:
        share = pl.pallas_call(
            functools.partial(share_kernel, grad_scale),
            out_shape=shape((group, share_rows, width), bf16),
            in_specs=[VMEM] * 2,
            out_specs=VMEM,
            compiler_params=room(4),
            name="share",
        )(cross, other)
        owned = pl.pallas_call(
            functools.partial(slots_kernel, group, grad_scale),
            out_shape=shape((tokens + GAIN_ROWS, width), bf16),
            in_specs=[VMEM] * 3,
            out_specs=VMEM,
            cost_estimate=estimate(tokens * width, 4 * tokens * width),
            compiler_params=room(4),
            name="slots",
        )(mine, theirs, other_slots)
    else:
        total = (cross.astype(f32) + other.astype(f32)) * grad_scale
        share = jnp.broadcast_to(total.astype(bf16)[None], (group, share_rows, width))
        gains = theirs[half_slots:].astype(f32) + other_slots[half_slots:].astype(f32)
        gains = as_two((gains[:2] + gains[2:4]) * grad_scale)
        by_half = jnp.stack([mine, other_slots[:half_slots]])
        by_half = jnp.where(half == 0, by_half, by_half[::-1]).reshape(tokens, width)
        owned = jnp.concatenate([by_half, gains.astype(bf16), padding], axis=0)

    gathered = lax.all_to_all(
        share, both, split_axis=0, concat_axis=0, tiled=True, axis_index_groups=half_groups
    )

    wanted_all = from_all(wanted, replicas)
    owned_all = from_all(owned, replicas)
    lanes = 128
    block = min(rows_dev, 2048 // replicas)
    row_update, state_new, grad_gains = pl.pallas_call(
        functools.partial(adagrad_kernel, twist, replicas),
        grid=(rows_dev // block,),
        out_shape=(
            shape((rows_dev, width), f32),
            shape((rows_dev // lanes, 1, lanes), f32),
            shape((2, width), f32),
        ),
        in_specs=[pl.BlockSpec((1, tokens), lambda step: (0, 0))] * replicas
        + [pl.BlockSpec((tokens + GAIN_ROWS, width), lambda step: (0, 0))] * replicas
        + [pl.BlockSpec((block // lanes, 1, lanes), lambda step: (step, 0, 0))],
        out_specs=(
            pl.BlockSpec((block, width), lambda step: (step, 0)),
            pl.BlockSpec((block // lanes, 1, lanes), lambda step: (step, 0, 0)),
            pl.BlockSpec((2, width), lambda step: (0, 0)),
        ),
        cost_estimate=estimate(2 * replicas * tokens * rows_dev * width, rows_dev * width * 4),
        compiler_params=room(12),
        name="adagrad",
    )(*wanted_all, *owned_all, adagrad_state.reshape(rows_dev // lanes, 1, lanes))

    halves = hand_on([gathered.reshape(part_rows, width)] * replicas)
    grads = ()
    for step, half in enumerate(halves):
        grads = pl.pallas_call(
            functools.partial(spread_kernel, twist, group, step, replicas),
            out_shape=(shape(w_uvqk.shape, f32), shape(w_out.shape, f32)),
            in_specs=[VMEM] + [pl.BlockSpec(memory_space=pl.ANY)] * len(grads),
            out_specs=(pl.BlockSpec(memory_space=pl.ANY),) * 2,
            scratch_shapes=[
                pltpu.VMEM((width // replicas, w_uvqk.shape[1]), f32),
                pltpu.VMEM((width // replicas, width), f32),
                pltpu.SemaphoreType.DMA((2,)),
            ],
            input_output_aliases={1: 0, 2: 1} if grads else {},
            cost_estimate=estimate(blocks * width * width, 3 * blocks * width * width),
            compiler_params=room(6),
        )(half, *grads)
    return (row_update, state_new.reshape(rows_dev), *grads, grad_gains)


def solution(mesh):
    placed = (
        P("replica", "shard", None),
        P("replica", "shard"),
        P("replica", "shard", None),
        P("replica", "shard", None),
        P("shard", None),
        P("shard"),
        P(),
        P(),
        P(),
        P(),
    )

    return jax.shard_map(
        on_device,
        mesh=mesh,
        in_specs=placed,
        out_specs=(P("shard", None), P("shard"), P(), P(), P()),
        check_vma=False,
    )
```
